32 devices in a mesh: section: 2 (over y), dp: 16 (over z, x, core).
Axes of the slice: x: 2, y: 2, z: 4, core: 2. Of those that a mesh axis runs over, the one named last changes fastest.
Arguments:
- activations: bfloat16 [2, 4, 16, 14336], P('section', None, 'dp'), may hold values from -6 to 6
- out_grads: bfloat16 [2, 4, 16, 4096], P('section', None, 'dp'), may hold values from -6 to 6
- basis_in: bfloat16 [2, 14336, 1024], P('section', 'dp'), may hold values from -0.046875 to 0.046875
- basis_out: bfloat16 [2, 4096, 1024], P('section', 'dp'), may hold values from -0.09375 to 0.09375
- eigen_values: float32 [2, 1024, 1024], P('section', 'dp'), may hold values from 0.02 to 2
- query_proj: bfloat16 [2, 8, 1024, 1024], P('section', None, 'dp'), may hold values from -0.046875 to 0.046875
- lengths: int32 [4], replicated, may hold values from 4 to 16
- seq_rows: int32 [4], replicated, may hold values from 0 to 127
- prior_table: float32 [128, 8], P('dp'), may hold values from -6 to 6
Outputs:
- influence: float32 [2, 128, 8], P('section', 'dp')
The draws below stay inside these ranges and needn't reach their ends.
All inputs are finite; a program needn't handle non-finite values.
Results may differ from the reference program's by a relative error of at most 0.01.
Values may be sent and summed in bfloat16 or wider, within the bound.
No kernel may reach another device: no remote copies, remote signals or barrier semaphores. Data moves between devices by JAX's collectives and lax.ppermute only.
A program may use at most 64 MiB of HBM per device.

```python
import math
import jax
import jax.numpy as jnp
from jax import lax

D = 4096
FFW = 14336
RANK = 1024
QUERIES = 8
MB = 4
SECTIONS = 2
SLOTS = 16
TABLE = 128


def with_ends(values, stream_key, low, largest):
    spot = [jax.random.randint(jax.random.fold_in(stream_key, axis), (), 0, length) for axis, length in enumerate(values.shape)]
    widest = values.shape.index(max(values.shape))
    neighbour = spot[:widest] + [(spot[widest] + 1) % values.shape[widest]] + spot[widest + 1:]
    return values.at[tuple(spot)].set(low).at[tuple(neighbour)].set(largest)


def shard_levels(key, dims, pieces, low, top_value):
    level = 1.0
    for dim, shards_of in pieces:
        steps = jax.random.uniform(jax.random.fold_in(jax.random.fold_in(key, 6), dim), (shards_of,), jnp.float32, low / len(pieces), top_value / len(pieces))
        level = level * jnp.repeat(jnp.exp(steps), dims[dim] // shards_of).reshape((-1,) + (1,) * (len(dims) - 1 - dim))
    return level


def normal_values(own_key, shape, spread, reach, pieces=(), kind=jnp.bfloat16):
    drawn = jax.random.normal(own_key, shape, jnp.float32) * spread
    if len(pieces) > 0:
        drawn = shard_levels(own_key, shape, pieces, -0.22, 0.18) * drawn
    return jnp.clip(drawn, min=-reach, max=reach).astype(kind)


def setup_inputs(seed: int = 0) -> dict:
    key_list = jax.random.split(jax.random.key(seed), 10)
    activations = normal_values(key_list[0], (SECTIONS, MB, SLOTS, FFW), 1.0, 6.0, ((0, 2), (2, 16)))
    out_grads = normal_values(key_list[1], (SECTIONS, MB, SLOTS, D), 1.0, 6.0, ((0, 2), (2, 16)))
    basis_in = normal_values(key_list[2], (SECTIONS, FFW, RANK), FFW ** -0.5, 0.046875, ((0, 2), (1, 16)))
    basis_out = normal_values(key_list[3], (SECTIONS, D, RANK), D ** -0.5, 0.09375, ((0, 2), (1, 16)))
    eigen_values = jnp.clip(jnp.exp(math.log(2.0) - 4.6051702 * jax.random.uniform(key_list[4], (SECTIONS, RANK, RANK), jnp.float32) ** shard_levels(key_list[4], (SECTIONS, RANK, RANK), ((0, 2), (1, 16)), -0.2, 0.2)), 0.02, 2.0)
    query_proj = normal_values(key_list[5], (SECTIONS, QUERIES, RANK, RANK), (RANK * RANK // 64) ** -0.5, 0.046875, ((0, 2), (2, 16)))
    lengths = with_ends(jax.random.randint(key_list[6], (MB,), SLOTS // 4, SLOTS + 1), jax.random.fold_in(key_list[6], 1), SLOTS // 4, SLOTS).astype(jnp.int32)
    seq_rows = with_ends(jax.random.randint(key_list[7], (MB,), 0, TABLE), jax.random.fold_in(key_list[7], 1), 0, TABLE - 1).astype(jnp.int32)
    prior_table = normal_values(key_list[8], (TABLE, QUERIES), 1.0, 6.0, ((0, 16),), jnp.float32)
    return dict(activations=activations, out_grads=out_grads, basis_in=basis_in, basis_out=basis_out, eigen_values=eigen_values, query_proj=query_proj, lengths=lengths, seq_rows=seq_rows, prior_table=prior_table)


DAMPING = 0.01


def reference(activations, out_grads, basis_in, basis_out, eigen_values, query_proj, lengths, seq_rows, prior_table):
    position = jnp.arange(SLOTS, dtype=jnp.int32)
    live_mask = (position[None, :] < lengths[:, None]).reshape(MB * SLOTS, 1)
    inverse_len = 1.0 / lengths.astype(jnp.float32)
    owner_mask = (seq_rows[None, :] == jnp.arange(TABLE, dtype=jnp.int32)[:, None]).astype(jnp.float32)
    running = jnp.zeros((MB, QUERIES), jnp.float32)
    layers_out = []
    for section_index in range(SECTIONS):
        act_proj = jnp.dot(activations[section_index].reshape(MB * SLOTS, FFW), basis_in[section_index], preferred_element_type=jnp.float32).astype(jnp.bfloat16)
        grad_proj = jnp.dot(out_grads[section_index].reshape(MB * SLOTS, D), basis_out[section_index], preferred_element_type=jnp.float32).astype(jnp.bfloat16)
        grad_proj = jnp.where(live_mask, grad_proj, jnp.zeros_like(grad_proj))
        act_proj = lax.optimization_barrier(act_proj)
        grad_proj = lax.optimization_barrier(grad_proj)
        seq_grad = jnp.einsum("mti,mtj->mij", grad_proj.astype(jnp.float32).reshape(MB, SLOTS, RANK), act_proj.astype(jnp.float32).reshape(MB, SLOTS, RANK), precision=lax.Precision.HIGHEST)
        seq_grad = seq_grad * inverse_len[:, None, None]
        precond = (query_proj[section_index].astype(jnp.float32) / (eigen_values[section_index][None] + DAMPING)).astype(jnp.bfloat16)
        precond = lax.optimization_barrier(precond).astype(jnp.float32)
        layer_score = jnp.dot(seq_grad.reshape(MB, RANK * RANK), precond.reshape(QUERIES, RANK * RANK).T, precision=lax.Precision.HIGHEST)
        running = running + layer_score
        layers_out.append(prior_table + jnp.dot(owner_mask, running, precision=lax.Precision.HIGHEST))
    return jnp.stack(layers_out)
```

```python
import jax
import jax.numpy as jnp
from jax import lax
from jax.sharding import PartitionSpec as P

DAMPING = 0.01
F32 = jnp.float32
BF16 = jnp.bfloat16


def exchange(pieces, axes):
    return lax.all_to_all(pieces, axes, split_axis=0, concat_axis=0, tiled=True)


def per_device(
    activations,
    out_grads,
    basis_in,
    basis_out,
    eigen_values,
    query_proj,
    lengths,
    seq_rows,
    prior_table,
):
    n = lax.axis_size("dp")
    sections = lax.axis_size("section")
    micro, own_slots, hidden = activations.shape[1:]
    features = out_grads.shape[3]
    hidden_share, feature_share = hidden // n, features // n
    own_rows = micro * own_slots
    rows = n * own_rows
    rank = basis_in.shape[2]
    share = rank // n
    queries = query_proj.shape[1]

    pieces = jnp.concatenate(
        [
            activations[0].reshape(own_rows, n, hidden_share),
            out_grads[0].reshape(own_rows, n, feature_share),
        ],
        axis=2,
    ).transpose(1, 0, 2)
    got = exchange(pieces, "dp").reshape(rows, hidden_share + feature_share)

    act_part = jnp.dot(got[:, :hidden_share], basis_in[0], preferred_element_type=F32)
    grad_part = jnp.dot(got[:, hidden_share:], basis_out[0], preferred_element_type=F32)
    parts = jnp.concatenate(
        [
            act_part.astype(BF16).reshape(rows, n, share),
            grad_part.astype(BF16).reshape(rows, n, share),
        ],
        axis=2,
    ).transpose(1, 0, 2)
    sums = jnp.sum(exchange(parts, "dp").astype(F32), axis=0)
    act_own = sums[:, :share].astype(BF16)

    row = jnp.arange(rows, dtype=jnp.int32)
    row_micro = (row // own_slots) % micro
    row_slot = (row // own_rows) * own_slots + row % own_slots
    micro_mask = row_micro[None, :] == jnp.arange(micro, dtype=jnp.int32)[:, None]
    live = jnp.any(micro_mask & (row_slot[None, :] < lengths[:, None]), axis=0)
    grad_own = jnp.where(live[:, None], sums[:, share:], 0.0).astype(BF16)

    act_all = exchange(jnp.broadcast_to(act_own[None], (n, rows, share)), "dp")
    act_proj = act_all.transpose(1, 0, 2).reshape(rows, rank)

    precond = (query_proj[0].astype(F32) / (eigen_values[0][None] + DAMPING)).astype(BF16)
    turned = jnp.einsum("ri,qij->qrj", grad_own, precond, preferred_element_type=F32)
    per_row = jnp.sum(turned * act_proj.astype(F32)[None], axis=2)
    weight = micro_mask.astype(F32) / lengths.astype(F32)[:, None]
    partial = jnp.sum(per_row[None] * weight[:, None, :], axis=2)

    total = n * sections
    spread = jnp.broadcast_to(partial.reshape(1, 1, micro * queries), (total, 1, micro * queries))
    scores = exchange(spread, ("section", "dp"))
    sender_section = jnp.arange(total, dtype=jnp.int32) // n
    counted = sender_section <= lax.axis_index("section")
    depth = jnp.sum(jnp.where(counted[:, None, None], scores, 0.0), axis=(0, 1))
    depth = depth.reshape(micro, queries)

    table_rows = prior_table.shape[0]
    first_row = lax.axis_index("dp") * table_rows
    own = first_row + jnp.arange(table_rows, dtype=jnp.int32)
    owner_mask = (seq_rows[None, :] == own[:, None]).astype(F32)
    result = prior_table + jnp.sum(owner_mask[:, :, None] * depth[None], axis=1)
    return result[None]


def solution(mesh):
    return jax.shard_map(
        per_device,
        mesh=mesh,
        in_specs=(
            P("section", None, "dp", None),
            P("section", None, "dp", None),
            P("section", "dp", None),
            P("section", "dp", None),
            P("section", "dp", None),
            P("section", None, "dp", None),
            P(),
            P(),
            P("dp", None),
        ),
        out_specs=P("section", "dp", None),
        check_vma=False,
    )
```

```python
import functools

import jax
import jax.numpy as jnp
from jax import lax
from jax.experimental import pallas as pl
from jax.experimental.pallas import tpu as pltpu
from jax.sharding import PartitionSpec as P

DAMPING = 0.01
F32 = jnp.float32
BF16 = jnp.bfloat16
LANES = 128
VMEM = pl.BlockSpec(memory_space=pltpu.VMEM)


def exchange(pieces, axes):
    return lax.all_to_all(pieces, axes, split_axis=0, concat_axis=0, tiled=True)


def call(body, out_shapes, *operands):
    many = isinstance(out_shapes, (list, tuple))
    return pl.pallas_call(
        body,
        out_shape=out_shapes,
        in_specs=[VMEM] * len(operands),
        out_specs=[VMEM] * len(out_shapes) if many else VMEM,
        compiler_params=pltpu.CompilerParams(vmem_limit_bytes=16 << 20),
    )(*operands)


def place(peer, extra, rank):
    across = rank // LANES
    return pl.ds(peer // across * extra, extra), pl.ds(peer % across * LANES, LANES)


def prep_kernel(lengths_ref, *refs):
    eigen_hbm, query_hbm, grads_hbm, basis_hbm, kept_ref, precond_ref, weight_ref = refs[:7]
    query_ref, eigen_ref, grads_ref, sems = refs[7:]
    depth, rank = basis_hbm.shape
    copies = [
        pltpu.make_async_copy(source, target, sems.at[index])
        for index, (source, target) in enumerate(
            (
                (eigen_hbm, eigen_ref),
                (query_hbm, query_ref),
                (grads_hbm, grads_ref),
                (basis_hbm, kept_ref.at[:depth]),
            )
        )
    ]
    for copy in copies:
        copy.start()
    shape = weight_ref.shape
    micro = lengths_ref.shape[1]
    row = lax.broadcasted_iota(jnp.int32, shape, 0)
    slot, member = row // micro, row % micro
    length = jnp.zeros(shape, jnp.int32)
    for index in range(micro):
        length = jnp.where(member == index, lengths_ref[:, index : index + 1], length)
    weight_ref[...] = jnp.where(slot < length, 1.0 / length.astype(F32), 0.0)
    copies[0].wait()
    copies[1].wait()
    damped = eigen_ref[...] + DAMPING
    for query in range(query_ref.shape[0]):
        precond_ref[query] = (query_ref[query].astype(F32) / damped).astype(BF16)
    copies[2].wait()
    own_rows, features = grads_ref.shape
    extra = 2 * own_rows
    tail = kept_ref.at[depth:]
    for peer in range(features // (2 * LANES)):
        first = peer * 2 * LANES
        left = grads_ref[:, first : first + LANES]
        right = grads_ref[:, first + LANES : first + 2 * LANES]
        tail[place(peer, extra, rank)] = jnp.concatenate([left, right], axis=0)
    copies[3].wait()


def act_kernel(rows_ref, kept_ref, out_ref):
    peers, own_rows, share = rows_ref.shape
    acts = rows_ref[...].reshape(peers * own_rows, share)
    part = jnp.dot(acts, kept_ref[:share], preferred_element_type=F32).astype(BF16)
    rank = part.shape[1]
    blocks = rank // LANES
    height = part.shape[0] * blocks // peers
    for peer in range(peers):
        group, block = peer // blocks, peer % blocks
        out_ref[peer, :height] = part[
            group * height : (group + 1) * height, block * LANES : (block + 1) * LANES
        ]
        out_ref[peer, height:] = kept_ref.at[share:][place(peer, 2 * own_rows, rank)]


def halves(top, bottom, low):
    return (
        jnp.where(low, top, pltpu.roll(bottom, LANES // 2, 1)),
        jnp.where(low, pltpu.roll(top, LANES // 2, 1), bottom),
    )


def grad_kernel(height, got_ref, basis_ref, out_ref):
    peers = got_ref.shape[0]
    total = got_ref[0, :height].astype(F32)
    for peer in range(1, peers):
        total += got_ref[peer, :height].astype(F32)
    total = total.astype(BF16)
    upper = lax.broadcasted_iota(jnp.int32, (8, LANES), 0) < 4
    left, right = [], []
    for pair in range(peers // 2):
        one = got_ref[2 * pair, height:].astype(F32)
        two = got_ref[2 * pair + 1, height:].astype(F32)
        left.append(jnp.where(upper, one, pltpu.roll(two, 4, 0)))
        right.append(jnp.where(upper, pltpu.roll(one, 4, 0), two))
    grads = jnp.concatenate(
        [jnp.concatenate(left, axis=0), jnp.concatenate(right, axis=0)], axis=1
    ).astype(BF16)
    part = jnp.dot(grads, basis_ref[...], preferred_element_type=F32)
    half = part.shape[0] // 2
    low = lax.broadcasted_iota(jnp.int32, (half, LANES), 1) < LANES // 2
    for block in range(peers // 2):
        at = block * LANES
        one, two = halves(part[:half, at : at + LANES], part[half:, at : at + LANES], low)
        for peer, piece in ((2 * block, one), (2 * block + 1, two)):
            out_ref[peer, :height] = total
            out_ref[peer, height:] = piece.astype(BF16)


def score_kernel(height, got_ref, precond_ref, weight_ref, *refs):
    out_ref = refs[-1]
    peers = got_ref.shape[0]
    queries, share, rank = precond_ref.shape
    rows = weight_ref.shape[0]
    blocks = rank // LANES
    packed = got_ref[0, height:].astype(F32)
    for peer in range(1, peers):
        packed += got_ref[peer, height:].astype(F32)
    grads = jnp.concatenate(
        [packed[:, :share], pltpu.roll(packed, share, 1)[:, :share]], axis=0
    ).astype(BF16)
    lane = lax.broadcasted_iota(jnp.int32, (8, LANES), 1)
    member = lax.broadcasted_iota(jnp.int32, (8, LANES), 0)
    held = jnp.zeros((8, LANES), F32)
    for query in range(queries):
        turned = jnp.dot(grads, precond_ref[query], preferred_element_type=F32)
        both = jnp.zeros((8, LANES), F32)
        for group in range(rows // height):
            top = group * height
            acc = jnp.zeros((height, LANES), F32)
            for block in range(blocks):
                piece = turned[top : top + height, block * LANES : (block + 1) * LANES]
                acc += piece * got_ref[group * blocks + block, :height].astype(F32)
            acc *= weight_ref[top : top + height]
            for first in range(0, height, 8):
                both += acc[first : first + 8]
        value = jnp.sum(both + pltpu.roll(both, 4, 0), axis=1, keepdims=True)
        held = jnp.where(lane == member * queries + query, value, held)
    held = jnp.where(member < 4, held, 0.0)
    line = jnp.broadcast_to(jnp.sum(held, axis=0, keepdims=True), held.shape)
    for first in range(0, out_ref.shape[0], 8):
        out_ref[first : first + 8] = line


def table_kernel(per_section, queries, got_ref, rows_ref, prior_ref, out_ref):
    sender = lax.broadcasted_iota(jnp.int32, got_ref.shape, 0) // per_section
    counted = sender <= lax.axis_index("section")
    depth = jnp.sum(jnp.where(counted, got_ref[...], 0.0), axis=0, keepdims=True)
    shape = prior_ref.shape
    own = lax.axis_index("dp") * shape[0] + lax.broadcasted_iota(jnp.int32, shape, 0)
    table = prior_ref[...]
    for member in range(rows_ref.shape[1]):
        first = member * queries
        scores = jnp.broadcast_to(depth[:, first : first + queries], shape)
        table += jnp.where(rows_ref[:, member : member + 1] == own, scores, 0.0)
    out_ref[0] = table


def packed_path(
    activations,
    out_grads,
    basis_in,
    basis_out,
    eigen_values,
    query_proj,
    lengths,
    seq_rows,
    prior_table,
):
    n, sections = lax.axis_size("dp"), lax.axis_size("section")
    micro, own_slots, hidden = activations.shape[1:]
    features = out_grads.shape[3]
    own_rows = micro * own_slots
    rows = n * own_rows
    rank = basis_in.shape[2]
    queries = query_proj.shape[1]
    height = rows * rank // (n * LANES)
    extra = own_rows * features // (n * LANES)

    lengths, seq_rows = lengths[None], seq_rows[None]
    grads = out_grads[0].reshape(own_rows, features)

    pieces = activations[0].reshape(own_rows, n, hidden // n).transpose(1, 0, 2)
    got = exchange(pieces, "dp")
    sources = (eigen_values[0], query_proj[0], grads, basis_in[0])
    kept, precond, weight = pl.pallas_call(
        prep_kernel,
        out_shape=[
            jax.ShapeDtypeStruct((hidden // n + n * extra * LANES // rank, rank), BF16),
            jax.ShapeDtypeStruct(query_proj.shape[1:], BF16),
            jax.ShapeDtypeStruct((rows, LANES), F32),
        ],
        in_specs=[VMEM] + [pl.BlockSpec(memory_space=pltpu.HBM)] * len(sources),
        out_specs=[VMEM] * 3,
        scratch_shapes=[
            pltpu.VMEM(query_proj.shape[1:], BF16),
            pltpu.VMEM(eigen_values.shape[1:], F32),
            pltpu.VMEM((own_rows, features), BF16),
            pltpu.SemaphoreType.DMA((len(sources),)),
        ],
        compiler_params=pltpu.CompilerParams(vmem_limit_bytes=16 << 20),
    )(lengths, *(pltpu.with_memory_space_constraint(array, pltpu.HBM) for array in sources))
    parts = call(
        act_kernel,
        jax.ShapeDtypeStruct((n, height + extra, LANES), BF16),
        got,
        kept,
    )
    parts = exchange(parts, "dp")
    parts = call(
        functools.partial(grad_kernel, height),
        jax.ShapeDtypeStruct((n, 2 * height, LANES), BF16),
        parts,
        basis_out[0],
    )
    parts = exchange(parts, "dp")
    total = n * sections
    spread = call(
        functools.partial(score_kernel, height),
        jax.ShapeDtypeStruct((total, LANES), F32),
        parts,
        precond,
        weight,
        seq_rows,
        prior_table,
    )
    scores = exchange(spread.reshape(total, 1, LANES), ("section", "dp")).reshape(total, LANES)
    return call(
        functools.partial(table_kernel, n, queries),
        jax.ShapeDtypeStruct((1,) + prior_table.shape, F32),
        scores,
        seq_rows,
        prior_table,
    )


def general_path(
    activations,
    out_grads,
    basis_in,
    basis_out,
    eigen_values,
    query_proj,
    lengths,
    seq_rows,
    prior_table,
):
    n = lax.axis_size("dp")
    sections = lax.axis_size("section")
    micro, own_slots, hidden = activations.shape[1:]
    features = out_grads.shape[3]
    hidden_share, feature_share = hidden // n, features // n
    own_rows = micro * own_slots
    rows = n * own_rows
    rank = basis_in.shape[2]
    share = rank // n
    queries = query_proj.shape[1]

    pieces = jnp.concatenate(
        [
            activations[0].reshape(own_rows, n, hidden_share),
            out_grads[0].reshape(own_rows, n, feature_share),
        ],
        axis=2,
    ).transpose(1, 0, 2)
    got = exchange(pieces, "dp").reshape(rows, hidden_share + feature_share)

    act_part = jnp.dot(got[:, :hidden_share], basis_in[0], preferred_element_type=F32)
    grad_part = jnp.dot(got[:, hidden_share:], basis_out[0], preferred_element_type=F32)
    parts = jnp.concatenate(
        [
            act_part.astype(BF16).reshape(rows, n, share),
            grad_part.astype(BF16).reshape(rows, n, share),
        ],
        axis=2,
    ).transpose(1, 0, 2)
    sums = jnp.sum(exchange(parts, "dp").astype(F32), axis=0)
    act_own = sums[:, :share].astype(BF16)

    row = jnp.arange(rows, dtype=jnp.int32)
    row_micro = (row // own_slots) % micro
    row_slot = (row // own_rows) * own_slots + row % own_slots
    micro_mask = row_micro[None, :] == jnp.arange(micro, dtype=jnp.int32)[:, None]
    live = jnp.any(micro_mask & (row_slot[None, :] < lengths[:, None]), axis=0)
    grad_own = jnp.where(live[:, None], sums[:, share:], 0.0).astype(BF16)

    act_all = exchange(jnp.broadcast_to(act_own[None], (n, rows, share)), "dp")
    act_proj = act_all.transpose(1, 0, 2).reshape(rows, rank)

    precond = (query_proj[0].astype(F32) / (eigen_values[0][None] + DAMPING)).astype(BF16)
    turned = jnp.einsum("ri,qij->qrj", grad_own, precond, preferred_element_type=F32)
    per_row = jnp.sum(turned * act_proj.astype(F32)[None], axis=2)
    weight = micro_mask.astype(F32) / lengths.astype(F32)[:, None]
    partial = jnp.sum(per_row[None] * weight[:, None, :], axis=2)

    total = n * sections
    spread = jnp.broadcast_to(partial.reshape(1, 1, micro * queries), (total, 1, micro * queries))
    scores = exchange(spread, ("section", "dp"))
    sender_section = jnp.arange(total, dtype=jnp.int32) // n
    counted = sender_section <= lax.axis_index("section")
    depth = jnp.sum(jnp.where(counted[:, None, None], scores, 0.0), axis=(0, 1))
    depth = depth.reshape(micro, queries)

    table_rows = prior_table.shape[0]
    first_row = lax.axis_index("dp") * table_rows
    own = first_row + jnp.arange(table_rows, dtype=jnp.int32)
    owner_mask = (seq_rows[None, :] == own[:, None]).astype(F32)
    result = prior_table + jnp.sum(owner_mask[:, :, None] * depth[None], axis=1)
    return result[None]


def per_device(*arrays):
    activations, out_grads, basis_in, _, _, query_proj, _, _, prior_table = arrays
    n = lax.axis_size("dp")
    micro, own_slots, hidden = activations.shape[1:]
    features = out_grads.shape[3]
    rank = basis_in.shape[2]
    queries = query_proj.shape[1]
    packs = (
        micro == 4
        and own_slots == 1
        and n % 8 == 0
        and hidden % (n * LANES) == 0
        and features == 2 * n * LANES
        and 2 * rank == n * LANES
        and micro * queries <= LANES
        and prior_table.shape[0] % 8 == 0
    )
    return (packed_path if packs else general_path)(*arrays)


def solution(mesh):
    return jax.shard_map(
        per_device,
        mesh=mesh,
        in_specs=(
            P("section", None, "dp", None),
            P("section", None, "dp", None),
            P("section", "dp", None),
            P("section", "dp", None),
            P("section", "dp", None),
            P("section", None, "dp", None),
            P(),
            P(),
            P("dp", None),
        ),
        out_specs=P("section", "dp", None),
        check_vma=False,
    )
```

```python
import functools

import jax
import jax.numpy as jnp
from jax import lax
from jax.experimental import pallas as pl
from jax.experimental.pallas import tpu as pltpu
from jax.sharding import PartitionSpec as P


DAMPING = 0.01
F32 = jnp.float32
BF16 = jnp.bfloat16
LANES = 128
VMEM = pl.BlockSpec(memory_space=pltpu.VMEM)


def exchange(pieces, axes):
    return lax.all_to_all(pieces, axes, split_axis=0, concat_axis=0, tiled=True)


def call(body, out_shapes, *operands):
    many = isinstance(out_shapes, (list, tuple))
    return pl.pallas_call(
        body,
        out_shape=out_shapes,
        in_specs=[VMEM] * len(operands),
        out_specs=[VMEM] * len(out_shapes) if many else VMEM,
        compiler_params=pltpu.CompilerParams(vmem_limit_bytes=16 << 20),
    )(*operands)


def pack_kernel(acts_hbm, grads_hbm, basis_hbm, out_ref, basis_ref, acts_ref, grads_ref, sems):
    copies = [
        pltpu.make_async_copy(acts_hbm, acts_ref, sems.at[0]),
        pltpu.make_async_copy(grads_hbm, grads_ref, sems.at[1]),
        pltpu.make_async_copy(basis_hbm, basis_ref, sems.at[2]),
    ]
    for copy in copies:
        copy.start()
    peers = out_ref.shape[0]
    hidden, features = acts_ref.shape[1] // peers, grads_ref.shape[1] // peers
    copies[0].wait()
    for peer in range(peers):
        out_ref[peer, :, :hidden] = acts_ref[:, peer * hidden : (peer + 1) * hidden]
    copies[1].wait()
    for peer in range(peers):
        out_ref[peer, :, hidden:] = grads_ref[:, peer * features : (peer + 1) * features]
    copies[2].wait()


def prep_kernel(lengths_ref, eigen_hbm, query_hbm, after_ref, *refs):
    del after_ref
    precond_ref, weight_ref, query_ref, eigen_ref, sems = refs
    copies = [
        pltpu.make_async_copy(eigen_hbm, eigen_ref, sems.at[0]),
        pltpu.make_async_copy(query_hbm, query_ref, sems.at[1]),
    ]
    for copy in copies:
        copy.start()
    shape = weight_ref.shape
    micro = lengths_ref.shape[1]
    row = lax.axis_index("dp") % 2 * shape[0] + lax.broadcasted_iota(jnp.int32, shape, 0)
    slot, member = row // micro, row % micro
    length = jnp.zeros(shape, jnp.int32)
    for index in range(micro):
        length = jnp.where(member == index, lengths_ref[:, index : index + 1], length)
    weight_ref[...] = jnp.where(slot < length, 1.0 / length.astype(F32), 0.0)
    for copy in copies:
        copy.wait()
    damped = eigen_ref[...] + DAMPING
    for query in range(query_ref.shape[0]):
        precond_ref[query] = (query_ref[query].astype(F32) / damped).astype(BF16)


def split_kernel(acts_ref, grads_ref, mine_ref, other_ref):
    half, rank = mine_ref.shape[0], acts_ref.shape[1]
    first = lax.axis_index("dp") % 2 == 0
    for at, part_ref in ((0, acts_ref), (rank, grads_ref)):
        top, bottom = part_ref[:half], part_ref[half:]
        mine_ref[:, at : at + rank] = jnp.where(first, top, bottom)
        other_ref[:, at : at + rank] = jnp.where(first, bottom, top)


def pair_kernel(mine_ref, got_ref, keep_ref, send_ref):
    total = mine_ref[...].astype(F32) + got_ref[...].astype(F32)
    rank = total.shape[1] // 2
    acts = total[:, :rank].astype(BF16)
    keep_ref[:, :rank] = acts
    send_ref[:, :rank] = acts
    first = lax.axis_index("dp") // 2 % 2 == 0
    for block in range(rank // (2 * LANES)):
        at = rank + 2 * block * LANES
        one, two = total[:, at : at + LANES], total[:, at + LANES : at + 2 * LANES]
        to = rank + block * LANES
        keep_ref[:, to : to + LANES] = jnp.where(first, one, two).astype(BF16)
        send_ref[:, to : to + LANES] = jnp.where(first, two, one).astype(BF16)


def plane_kernel(keep_ref, got_ref, out_ref):
    total = (keep_ref[...].astype(F32) + got_ref[...].astype(F32)).astype(BF16)
    peers, height, _ = out_ref.shape
    rows = total.shape[0]
    blocks = height // rows - 1
    for peer in range(peers):
        for block in range(blocks + 1):
            at = (block if block < blocks else blocks + peer) * LANES
            out_ref[peer, block * rows : (block + 1) * rows] = total[:, at : at + LANES]


def score_kernel(got_ref, own_ref, swapped_ref, weight_ref, *refs):
    out_ref = refs[-1]
    peers = got_ref.shape[0]
    queries, share, rank = own_ref.shape
    rows = weight_ref.shape[0]
    blocks = rank // LANES
    total = got_ref[0].astype(F32)
    for peer in range(1, peers):
        total += got_ref[peer].astype(F32)
    grads = total[blocks * rows :]
    turned_lanes = pltpu.roll(grads, share, 1)
    first = lax.axis_index("dp") % 2 == 0
    own = jnp.where(first, grads, turned_lanes)[:, :share].astype(BF16)
    swapped = jnp.where(first, turned_lanes, grads)[:, :share].astype(BF16)
    lane = lax.broadcasted_iota(jnp.int32, (8, LANES), 1)
    member = lax.broadcasted_iota(jnp.int32, (8, LANES), 0)
    held = jnp.zeros((8, LANES), F32)
    for query in range(queries):
        turned = jnp.dot(own, own_ref[query], preferred_element_type=F32)
        turned += jnp.dot(swapped, swapped_ref[query], preferred_element_type=F32)
        acc = jnp.zeros((rows, LANES), F32)
        for block in range(blocks):
            acts = total[block * rows : (block + 1) * rows]
            acc += turned[:, block * LANES : (block + 1) * LANES] * acts
        acc *= weight_ref[...]
        both = acc[:8]
        for at in range(8, rows, 8):
            both += acc[at : at + 8]
        value = jnp.sum(both + pltpu.roll(both, 4, 0), axis=1, keepdims=True)
        held = jnp.where(lane == member * queries + query, value, held)
    held = jnp.where(member < 4, held, 0.0)
    line = jnp.broadcast_to(jnp.sum(held, axis=0, keepdims=True), held.shape)
    for at in range(0, out_ref.shape[0], 8):
        out_ref[at : at + 8] = line


def table_kernel(per_section, queries, got_ref, rows_ref, prior_ref, out_ref):
    sender = lax.broadcasted_iota(jnp.int32, got_ref.shape, 0) // per_section
    counted = sender <= lax.axis_index("section")
    depth = jnp.sum(jnp.where(counted, got_ref[...], 0.0), axis=0, keepdims=True)
    shape = prior_ref.shape
    own = lax.axis_index("dp") * shape[0] + lax.broadcasted_iota(jnp.int32, shape, 0)
    table = prior_ref[...]
    for member in range(rows_ref.shape[1]):
        first = member * queries
        scores = jnp.broadcast_to(depth[:, first : first + queries], shape)
        table += jnp.where(rows_ref[:, member : member + 1] == own, scores, 0.0)
    out_ref[0] = table


def packed_path(
    activations,
    out_grads,
    basis_in,
    basis_out,
    eigen_values,
    query_proj,
    lengths,
    seq_rows,
    prior_table,
):
    n, sections = lax.axis_size("dp"), lax.axis_size("section")
    micro, own_slots, hidden = activations.shape[1:]
    features = out_grads.shape[3]
    own_rows = micro * own_slots
    half = n * own_rows // 2
    rank = basis_in.shape[2]
    width = (hidden + features) // n
    lengths, seq_rows = lengths[None], seq_rows[None]
    hbm = pl.BlockSpec(memory_space=pltpu.HBM)
    params = pltpu.CompilerParams(vmem_limit_bytes=16 << 20)

    def in_hbm(*arrays):
        return [pltpu.with_memory_space_constraint(array, pltpu.HBM) for array in arrays]

    def swap(value, bit):
        return lax.ppermute(value, "dp", [(i, i ^ bit) for i in range(n)])

    pieces, basis_out = pl.pallas_call(
        pack_kernel,
        out_shape=[
            jax.ShapeDtypeStruct((n, own_rows, width), BF16),
            jax.ShapeDtypeStruct(basis_out.shape[1:], BF16),
        ],
        in_specs=[hbm] * 3,
        out_specs=[VMEM] * 2,
        scratch_shapes=[
            pltpu.VMEM((own_rows, hidden), BF16),
            pltpu.VMEM((own_rows, features), BF16),
            pltpu.SemaphoreType.DMA((3,)),
        ],
        compiler_params=params,
    )(
        *in_hbm(
            activations[0].reshape(own_rows, hidden),
            out_grads[0].reshape(own_rows, features),
            basis_out[0],
        )
    )
    got = exchange(pieces, "dp").reshape(2 * half, width)
    share = hidden // n
    mine, other = call(
        split_kernel,
        [jax.ShapeDtypeStruct((half, 2 * rank), BF16)] * 2,
        jnp.dot(got[:, :share], basis_in[0], preferred_element_type=F32).astype(BF16),
        jnp.dot(got[:, share:], basis_out, preferred_element_type=F32).astype(BF16),
    )
    keep, send = call(
        pair_kernel,
        [jax.ShapeDtypeStruct((half, rank + rank // 2), BF16)] * 2,
        mine,
        swap(other, 1),
    )
    beside = swap(send, 2)
    prepare = pl.pallas_call(
        prep_kernel,
        out_shape=[
            jax.ShapeDtypeStruct(query_proj.shape[1:], BF16),
            jax.ShapeDtypeStruct((half, LANES), F32),
        ],
        in_specs=[VMEM, hbm, hbm, VMEM],
        out_specs=[VMEM] * 2,
        scratch_shapes=[
            pltpu.VMEM(query_proj.shape[1:], BF16),
            pltpu.VMEM(eigen_values.shape[1:], F32),
            pltpu.SemaphoreType.DMA((2,)),
        ],
        compiler_params=params,
    )
    precond, weight = prepare(lengths, *in_hbm(eigen_values[0], query_proj[0]), keep)
    swapped = swap(precond, 1)
    planes = n // 4
    parts = call(
        plane_kernel,
        jax.ShapeDtypeStruct((planes, half * (rank // LANES + 1), LANES), BF16),
        keep,
        beside,
    )
    parts = lax.all_to_all(
        parts,
        "dp",
        split_axis=0,
        concat_axis=0,
        tiled=True,
        axis_index_groups=[[4 * plane + spot for plane in range(planes)] for spot in range(4)],
    )
    total = n * sections
    spread = call(
        score_kernel,
        jax.ShapeDtypeStruct((total, LANES), F32),
        parts,
        precond,
        swapped,
        weight,
        seq_rows,
        prior_table,
    )
    scores = exchange(spread.reshape(total, 1, LANES), ("section", "dp")).reshape(total, LANES)
    return call(
        functools.partial(table_kernel, n, query_proj.shape[1]),
        jax.ShapeDtypeStruct((1,) + prior_table.shape, F32),
        scores,
        seq_rows,
        prior_table,
    )


def general_path(
    activations,
    out_grads,
    basis_in,
    basis_out,
    eigen_values,
    query_proj,
    lengths,
    seq_rows,
    prior_table,
):
    n = lax.axis_size("dp")
    sections = lax.axis_size("section")
    micro, own_slots, hidden = activations.shape[1:]
    features = out_grads.shape[3]
    hidden_share, feature_share = hidden // n, features // n
    own_rows = micro * own_slots
    rows = n * own_rows
    rank = basis_in.shape[2]
    share = rank // n
    queries = query_proj.shape[1]

    pieces = jnp.concatenate(
        [
            activations[0].reshape(own_rows, n, hidden_share),
            out_grads[0].reshape(own_rows, n, feature_share),
        ],
        axis=2,
    ).transpose(1, 0, 2)
    got = exchange(pieces, "dp").reshape(rows, hidden_share + feature_share)

    act_part = jnp.dot(got[:, :hidden_share], basis_in[0], preferred_element_type=F32)
    grad_part = jnp.dot(got[:, hidden_share:], basis_out[0], preferred_element_type=F32)
    parts = jnp.concatenate(
        [
            act_part.astype(BF16).reshape(rows, n, share),
            grad_part.astype(BF16).reshape(rows, n, share),
        ],
        axis=2,
    ).transpose(1, 0, 2)
    sums = jnp.sum(exchange(parts, "dp").astype(F32), axis=0)
    act_own = sums[:, :share].astype(BF16)

    row = jnp.arange(rows, dtype=jnp.int32)
    row_micro = (row // own_slots) % micro
    row_slot = (row // own_rows) * own_slots + row % own_slots
    micro_mask = row_micro[None, :] == jnp.arange(micro, dtype=jnp.int32)[:, None]
    live = jnp.any(micro_mask & (row_slot[None, :] < lengths[:, None]), axis=0)
    grad_own = jnp.where(live[:, None], sums[:, share:], 0.0).astype(BF16)

    act_all = exchange(jnp.broadcast_to(act_own[None], (n, rows, share)), "dp")
    act_proj = act_all.transpose(1, 0, 2).reshape(rows, rank)

    precond = (query_proj[0].astype(F32) / (eigen_values[0][None] + DAMPING)).astype(BF16)
    turned = jnp.einsum("ri,qij->qrj", grad_own, precond, preferred_element_type=F32)
    per_row = jnp.sum(turned * act_proj.astype(F32)[None], axis=2)
    weight = micro_mask.astype(F32) / lengths.astype(F32)[:, None]
    partial = jnp.sum(per_row[None] * weight[:, None, :], axis=2)

    total = n * sections
    spread = jnp.broadcast_to(partial.reshape(1, 1, micro * queries), (total, 1, micro * queries))
    scores = exchange(spread, ("section", "dp"))
    sender_section = jnp.arange(total, dtype=jnp.int32) // n
    counted = sender_section <= lax.axis_index("section")
    depth = jnp.sum(jnp.where(counted[:, None, None], scores, 0.0), axis=(0, 1))
    depth = depth.reshape(micro, queries)

    table_rows = prior_table.shape[0]
    first_row = lax.axis_index("dp") * table_rows
    own = first_row + jnp.arange(table_rows, dtype=jnp.int32)
    owner_mask = (seq_rows[None, :] == own[:, None]).astype(F32)
    result = prior_table + jnp.sum(owner_mask[:, :, None] * depth[None], axis=1)
    return result[None]


def per_device(*arrays):
    activations, out_grads, basis_in, _, _, query_proj, _, _, prior_table = arrays
    n = lax.axis_size("dp")
    micro, own_slots, hidden = activations.shape[1:]
    features = out_grads.shape[3]
    rank = basis_in.shape[2]
    queries = query_proj.shape[1]
    packs = (
        micro == 4
        and own_slots == 1
        and n % 8 == 0
        and hidden % (n * LANES) == 0
        and features % (n * LANES) == 0
        and 2 * rank == n * LANES
        and micro * queries <= LANES
        and prior_table.shape[0] % 8 == 0
    )
    return (packed_path if packs else general_path)(*arrays)


def solution(mesh):
    return jax.shard_map(
        per_device,
        mesh=mesh,
        in_specs=(
            P("section", None, "dp", None),
            P("section", None, "dp", None),
            P("section", "dp", None),
            P("section", "dp", None),
            P("section", "dp", None),
            P("section", None, "dp", None),
            P(),
            P(),
            P("dp", None),
        ),
        out_specs=P("section", "dp", None),
        check_vma=False,
    )
```

```python
import functools

import jax
import jax.numpy as jnp
from jax import lax
from jax.experimental import pallas as pl
from jax.experimental.pallas import tpu as pltpu
from jax.sharding import PartitionSpec as P


DAMPING = 0.01
F32 = jnp.float32
BF16 = jnp.bfloat16
LANES = 128
VMEM = pl.BlockSpec(memory_space=pltpu.VMEM)


def exchange(pieces, axes):
    return lax.all_to_all(pieces, axes, split_axis=0, concat_axis=0, tiled=True)


def call(body, out_shapes, *operands):
    many = isinstance(out_shapes, (list, tuple))
    return pl.pallas_call(
        body,
        out_shape=out_shapes,
        in_specs=[VMEM] * len(operands),
        out_specs=[VMEM] * len(out_shapes) if many else VMEM,
        compiler_params=pltpu.CompilerParams(vmem_limit_bytes=16 << 20),
    )(*operands)


def pack_kernel(acts_hbm, grads_hbm, basis_hbm, out_ref, basis_ref, acts_ref, grads_ref, sems):
    copies = [
        pltpu.make_async_copy(acts_hbm, acts_ref, sems.at[0]),
        pltpu.make_async_copy(grads_hbm, grads_ref, sems.at[1]),
        pltpu.make_async_copy(basis_hbm, basis_ref, sems.at[2]),
    ]
    for copy in copies:
        copy.start()
    peers = out_ref.shape[0]
    hidden, features = acts_ref.shape[1] // peers, grads_ref.shape[1] // peers
    copies[0].wait()
    for peer in range(peers):
        out_ref[peer, :, :hidden] = acts_ref[:, peer * hidden : (peer + 1) * hidden]
    copies[1].wait()
    for peer in range(peers):
        out_ref[peer, :, hidden:] = grads_ref[:, peer * features : (peer + 1) * features]
    copies[2].wait()


def prep_kernel(lengths_ref, eigen_hbm, query_hbm, after_ref, *refs):
    del after_ref
    precond_ref, weight_ref, query_ref, eigen_ref, sems = refs
    copies = [
        pltpu.make_async_copy(eigen_hbm, eigen_ref, sems.at[0]),
        pltpu.make_async_copy(query_hbm, query_ref, sems.at[1]),
    ]
    for copy in copies:
        copy.start()
    shape = weight_ref.shape
    micro = lengths_ref.shape[1]
    row = lax.axis_index("dp") % 2 * shape[0] + lax.broadcasted_iota(jnp.int32, shape, 0)
    slot, member = row // micro, row % micro
    length = jnp.zeros(shape, jnp.int32)
    for index in range(micro):
        length = jnp.where(member == index, lengths_ref[:, index : index + 1], length)
    weight_ref[...] = jnp.where(slot < length, 1.0 / length.astype(F32), 0.0)
    for copy in copies:
        copy.wait()
    damped = eigen_ref[...] + DAMPING
    for query in range(query_ref.shape[0]):
        precond_ref[query] = (query_ref[query].astype(F32) / damped).astype(BF16)


def split_kernel(acts_ref, grads_ref, mine_ref, other_ref):
    half, rank = mine_ref.shape[0], acts_ref.shape[1]
    first = lax.axis_index("dp") % 2 == 0
    for at, part_ref in ((0, acts_ref), (rank, grads_ref)):
        top, bottom = part_ref[:half], part_ref[half:]
        mine_ref[:, at : at + rank] = jnp.where(first, top, bottom)
        other_ref[:, at : at + rank] = jnp.where(first, bottom, top).astype(BF16)


def fold_kernel(bit, mine_ref, got_ref, keep_ref, send_ref):
    total = mine_ref[...] + got_ref[...].astype(F32)
    width = keep_ref.shape[1]
    rank = 2 * width - total.shape[1]
    acts = total[:, :rank]
    keep_ref[:, :rank] = acts
    send_ref[:, :rank] = acts.astype(BF16)
    first = lax.axis_index("dp") // bit % 2 == 0
    for to in range(rank, width, LANES):
        at = 2 * to - rank
        one, two = total[:, at : at + LANES], total[:, at + LANES : at + 2 * LANES]
        keep_ref[:, to : to + LANES] = jnp.where(first, one, two)
        send_ref[:, to : to + LANES] = jnp.where(first, two, one).astype(BF16)


def score_kernel(mine_ref, got_ref, own_ref, swapped_ref, weight_ref, *refs):
    out_ref = refs[-1]
    queries, share, rank = own_ref.shape
    rows = weight_ref.shape[0]
    blocks = rank // LANES
    total = mine_ref[...] + got_ref[...].astype(F32)
    grads = total[:, rank:]
    turned_lanes = pltpu.roll(grads, share, 1)
    first = lax.axis_index("dp") % 2 == 0
    sides = jnp.where(first, grads, turned_lanes).astype(BF16)
    lane = lax.broadcasted_iota(jnp.int32, (8, LANES), 1)
    member = lax.broadcasted_iota(jnp.int32, (8, LANES), 0)
    held = jnp.zeros((8, LANES), F32)
    for query in range(queries):
        precond = jnp.concatenate([own_ref[query], swapped_ref[query]], axis=0)
        turned = jnp.dot(sides, precond, preferred_element_type=F32)
        acc = jnp.zeros((rows, LANES), F32)
        for block in range(blocks):
            at = block * LANES
            acc += turned[:, at : at + LANES] * total[:, at : at + LANES]
        acc *= weight_ref[...]
        both = acc[:8]
        for at in range(8, rows, 8):
            both += acc[at : at + 8]
        value = jnp.sum(both + pltpu.roll(both, 4, 0), axis=1, keepdims=True)
        held = jnp.where(lane == member * queries + query, value, held)
    held = jnp.where(member < 4, held, 0.0)
    line = jnp.broadcast_to(jnp.sum(held, axis=0, keepdims=True), held.shape)
    for at in range(0, out_ref.shape[0], 8):
        out_ref[at : at + 8] = line


def table_kernel(per_section, queries, got_ref, rows_ref, prior_ref, out_ref):
    sender = lax.broadcasted_iota(jnp.int32, got_ref.shape, 0) // per_section
    counted = sender <= lax.axis_index("section")
    depth = jnp.sum(jnp.where(counted, got_ref[...], 0.0), axis=0, keepdims=True)
    shape = prior_ref.shape
    own = lax.axis_index("dp") * shape[0] + lax.broadcasted_iota(jnp.int32, shape, 0)
    table = prior_ref[...]
    for member in range(rows_ref.shape[1]):
        first = member * queries
        scores = jnp.broadcast_to(depth[:, first : first + queries], shape)
        table += jnp.where(rows_ref[:, member : member + 1] == own, scores, 0.0)
    out_ref[0] = table


def packed_path(
    activations,
    out_grads,
    basis_in,
    basis_out,
    eigen_values,
    query_proj,
    lengths,
    seq_rows,
    prior_table,
):
    n, sections = lax.axis_size("dp"), lax.axis_size("section")
    micro, own_slots, hidden = activations.shape[1:]
    features = out_grads.shape[3]
    own_rows = micro * own_slots
    half = n * own_rows // 2
    rank = basis_in.shape[2]
    width = (hidden + features) // n
    lengths, seq_rows = lengths[None], seq_rows[None]
    hbm = pl.BlockSpec(memory_space=pltpu.HBM)
    params = pltpu.CompilerParams(vmem_limit_bytes=16 << 20)

    def in_hbm(*arrays):
        return [pltpu.with_memory_space_constraint(array, pltpu.HBM) for array in arrays]

    def swap(value, bit):
        return lax.ppermute(value, "dp", [(i, i ^ bit) for i in range(n)])

    pieces, basis_out = pl.pallas_call(
        pack_kernel,
        out_shape=[
            jax.ShapeDtypeStruct((n, own_rows, width), BF16),
            jax.ShapeDtypeStruct(basis_out.shape[1:], BF16),
        ],
        in_specs=[hbm] * 3,
        out_specs=[VMEM] * 2,
        scratch_shapes=[
            pltpu.VMEM((own_rows, hidden), BF16),
            pltpu.VMEM((own_rows, features), BF16),
            pltpu.SemaphoreType.DMA((3,)),
        ],
        compiler_params=params,
    )(
        *in_hbm(
            activations[0].reshape(own_rows, hidden),
            out_grads[0].reshape(own_rows, features),
            basis_out[0],
        )
    )
    got = exchange(pieces, "dp").reshape(2 * half, width)
    share = hidden // n
    mine, other = call(
        split_kernel,
        [jax.ShapeDtypeStruct((half, 2 * rank), kind) for kind in (F32, BF16)],
        jnp.dot(got[:, :share], basis_in[0], preferred_element_type=F32),
        jnp.dot(got[:, share:], basis_out, preferred_element_type=F32),
    )
    keep, send, bit, prepared = mine, other, 1, None
    while bit < n:
        got = swap(send, bit)
        if bit == 2:
            prepared = keep
        bit *= 2
        if bit < n:
            kinds = (F32, BF16)
            width = rank + (keep.shape[1] - rank) // 2
            keep, send = call(
                functools.partial(fold_kernel, bit),
                [jax.ShapeDtypeStruct((half, width), kind) for kind in kinds],
                keep,
                got,
            )
    prepare = pl.pallas_call(
        prep_kernel,
        out_shape=[
            jax.ShapeDtypeStruct(query_proj.shape[1:], BF16),
            jax.ShapeDtypeStruct((half, LANES), F32),
        ],
        in_specs=[VMEM, hbm, hbm, VMEM],
        out_specs=[VMEM] * 2,
        scratch_shapes=[
            pltpu.VMEM(query_proj.shape[1:], BF16),
            pltpu.VMEM(eigen_values.shape[1:], F32),
            pltpu.SemaphoreType.DMA((2,)),
        ],
        compiler_params=params,
    )
    precond, weight = prepare(lengths, *in_hbm(eigen_values[0], query_proj[0]), prepared)
    swapped = swap(precond, 1)
    total = n * sections
    spread = call(
        score_kernel,
        jax.ShapeDtypeStruct((total, LANES), F32),
        keep,
        got,
        precond,
        swapped,
        weight,
        seq_rows,
        prior_table,
    )
    scores = exchange(spread.reshape(total, 1, LANES), ("section", "dp")).reshape(total, LANES)
    return call(
        functools.partial(table_kernel, n, query_proj.shape[1]),
        jax.ShapeDtypeStruct((1,) + prior_table.shape, F32),
        scores,
        seq_rows,
        prior_table,
    )


def general_path(
    activations,
    out_grads,
    basis_in,
    basis_out,
    eigen_values,
    query_proj,
    lengths,
    seq_rows,
    prior_table,
):
    n = lax.axis_size("dp")
    sections = lax.axis_size("section")
    micro, own_slots, hidden = activations.shape[1:]
    features = out_grads.shape[3]
    hidden_share, feature_share = hidden // n, features // n
    own_rows = micro * own_slots
    rows = n * own_rows
    rank = basis_in.shape[2]
    share = rank // n
    queries = query_proj.shape[1]

    pieces = jnp.concatenate(
        [
            activations[0].reshape(own_rows, n, hidden_share),
            out_grads[0].reshape(own_rows, n, feature_share),
        ],
        axis=2,
    ).transpose(1, 0, 2)
    got = exchange(pieces, "dp").reshape(rows, hidden_share + feature_share)

    act_part = jnp.dot(got[:, :hidden_share], basis_in[0], preferred_element_type=F32)
    grad_part = jnp.dot(got[:, hidden_share:], basis_out[0], preferred_element_type=F32)
    parts = jnp.concatenate(
        [
            act_part.astype(BF16).reshape(rows, n, share),
            grad_part.astype(BF16).reshape(rows, n, share),
        ],
        axis=2,
    ).transpose(1, 0, 2)
    sums = jnp.sum(exchange(parts, "dp").astype(F32), axis=0)
    act_own = sums[:, :share].astype(BF16)

    row = jnp.arange(rows, dtype=jnp.int32)
    row_micro = (row // own_slots) % micro
    row_slot = (row // own_rows) * own_slots + row % own_slots
    micro_mask = row_micro[None, :] == jnp.arange(micro, dtype=jnp.int32)[:, None]
    live = jnp.any(micro_mask & (row_slot[None, :] < lengths[:, None]), axis=0)
    grad_own = jnp.where(live[:, None], sums[:, share:], 0.0).astype(BF16)

    act_all = exchange(jnp.broadcast_to(act_own[None], (n, rows, share)), "dp")
    act_proj = act_all.transpose(1, 0, 2).reshape(rows, rank)

    precond = (query_proj[0].astype(F32) / (eigen_values[0][None] + DAMPING)).astype(BF16)
    turned = jnp.einsum("ri,qij->qrj", grad_own, precond, preferred_element_type=F32)
    per_row = jnp.sum(turned * act_proj.astype(F32)[None], axis=2)
    weight = micro_mask.astype(F32) / lengths.astype(F32)[:, None]
    partial = jnp.sum(per_row[None] * weight[:, None, :], axis=2)

    total = n * sections
    spread = jnp.broadcast_to(partial.reshape(1, 1, micro * queries), (total, 1, micro * queries))
    scores = exchange(spread, ("section", "dp"))
    sender_section = jnp.arange(total, dtype=jnp.int32) // n
    counted = sender_section <= lax.axis_index("section")
    depth = jnp.sum(jnp.where(counted[:, None, None], scores, 0.0), axis=(0, 1))
    depth = depth.reshape(micro, queries)

    table_rows = prior_table.shape[0]
    first_row = lax.axis_index("dp") * table_rows
    own = first_row + jnp.arange(table_rows, dtype=jnp.int32)
    owner_mask = (seq_rows[None, :] == own[:, None]).astype(F32)
    result = prior_table + jnp.sum(owner_mask[:, :, None] * depth[None], axis=1)
    return result[None]


def per_device(*arrays):
    activations, out_grads, basis_in, _, _, query_proj, _, _, prior_table = arrays
    n = lax.axis_size("dp")
    micro, own_slots, hidden = activations.shape[1:]
    features = out_grads.shape[3]
    rank = basis_in.shape[2]
    queries = query_proj.shape[1]
    packs = (
        micro == 4
        and own_slots == 1
        and n & (n - 1) == 0
        and n >= 8
        and hidden % (n * LANES) == 0
        and features % (n * LANES) == 0
        and 2 * rank == n * LANES
        and micro * queries <= LANES
        and prior_table.shape[0] % 8 == 0
    )
    return (packed_path if packs else general_path)(*arrays)


def solution(mesh):
    return jax.shard_map(
        per_device,
        mesh=mesh,
        in_specs=(
            P("section", None, "dp", None),
            P("section", None, "dp", None),
            P("section", "dp", None),
            P("section", "dp", None),
            P("section", "dp", None),
            P("section", None, "dp", None),
            P(),
            P(),
            P("dp", None),
        ),
        out_specs=P("section", "dp", None),
        check_vma=False,
    )
```

```python
import functools

import jax
import jax.numpy as jnp
from jax import lax
from jax.experimental import pallas as pl
from jax.experimental.pallas import tpu as pltpu
from jax.sharding import PartitionSpec as P


DAMPING = 0.01
F32 = jnp.float32
BF16 = jnp.bfloat16
LANES = 128
VMEM = pl.BlockSpec(memory_space=pltpu.VMEM)


def exchange(pieces, axes):
    return lax.all_to_all(pieces, axes, split_axis=0, concat_axis=0, tiled=True)


def call(body, out_shapes, *operands):
    many = isinstance(out_shapes, (list, tuple))
    return pl.pallas_call(
        body,
        out_shape=out_shapes,
        in_specs=[VMEM] * len(operands),
        out_specs=[VMEM] * len(out_shapes) if many else VMEM,
        compiler_params=pltpu.CompilerParams(vmem_limit_bytes=16 << 20),
    )(*operands)


def pack_kernel(acts_hbm, grads_hbm, basis_hbm, out_ref, basis_ref, acts_ref, grads_ref, sems):
    copies = [
        pltpu.make_async_copy(acts_hbm, acts_ref, sems.at[0]),
        pltpu.make_async_copy(grads_hbm, grads_ref, sems.at[1]),
        pltpu.make_async_copy(basis_hbm, basis_ref, sems.at[2]),
    ]
    for copy in copies:
        copy.start()
    peers = out_ref.shape[0]
    hidden, features = acts_ref.shape[1] // peers, grads_ref.shape[1] // peers
    copies[0].wait()
    for peer in range(peers):
        out_ref[peer, :, :hidden] = acts_ref[:, peer * hidden : (peer + 1) * hidden]
    copies[1].wait()
    for peer in range(peers):
        out_ref[peer, :, hidden:] = grads_ref[:, peer * features : (peer + 1) * features]
    copies[2].wait()


def prep_kernel(lengths_ref, eigen_hbm, query_hbm, after_ref, *refs):
    del after_ref
    precond_ref, weight_ref, query_ref, eigen_ref, sems = refs
    copies = [
        pltpu.make_async_copy(eigen_hbm, eigen_ref, sems.at[0]),
        pltpu.make_async_copy(query_hbm, query_ref, sems.at[1]),
    ]
    for copy in copies:
        copy.start()
    shape = weight_ref.shape
    micro = lengths_ref.shape[1]
    row = lax.axis_index("dp") % 2 * shape[0] + lax.broadcasted_iota(jnp.int32, shape, 0)
    slot, member = row // micro, row % micro
    length = jnp.zeros(shape, jnp.int32)
    for index in range(micro):
        length = jnp.where(member == index, lengths_ref[:, index : index + 1], length)
    weight_ref[...] = jnp.where(slot < length, 1.0 / length.astype(F32), 0.0)
    for copy in copies:
        copy.wait()
    damped = eigen_ref[...] + DAMPING
    for query in range(query_ref.shape[0]):
        precond_ref[query] = (query_ref[query].astype(F32) / damped).astype(BF16)


def split_kernel(acts_ref, grads_ref, mine_ref, other_ref):
    half, rank = mine_ref.shape[0], acts_ref.shape[1]
    first = lax.axis_index("dp") % 2 == 0
    for at, part_ref in ((0, acts_ref), (rank, grads_ref)):
        top, bottom = part_ref[:half], part_ref[half:]
        mine_ref[:, at : at + rank] = jnp.where(first, top, bottom)
        other_ref[:, at : at + rank] = jnp.where(first, bottom, top).astype(BF16)


def fold_kernel(bits, count, *refs):
    total = refs[0][...]
    for got_ref in refs[1:count]:
        total += got_ref[...].astype(F32)
    outs = refs[count:]
    ways = len(outs)
    width = outs[0].shape[1]
    blocks = (total.shape[1] - width) // LANES // (ways - 1)
    rank = width - blocks * LANES
    low = [lax.axis_index("dp") // bit % 2 == 0 for bit in bits]
    for offset, out_ref in enumerate(outs):
        out_ref[:, :rank] = total[:, :rank].astype(out_ref.dtype)
        for block in range(blocks):
            at = rank + block * ways * LANES
            left = [total[:, at + way * LANES : at + (way + 1) * LANES] for way in range(ways)]
            for place, mine in enumerate(low):
                flip = offset >> place & 1
                left = [
                    jnp.where(mine, left[pair + flip], left[pair + 1 - flip])
                    for pair in range(0, len(left), 2)
                ]
            to = rank + block * LANES
            out_ref[:, to : to + LANES] = left[0].astype(out_ref.dtype)


def score_kernel(mine_ref, got_ref, own_ref, swapped_ref, weight_ref, *refs):
    out_ref = refs[-1]
    queries, share, rank = own_ref.shape
    rows = weight_ref.shape[0]
    blocks = rank // LANES
    total = mine_ref[...] + got_ref[...].astype(F32)
    grads = total[:, rank:]
    turned_lanes = pltpu.roll(grads, share, 1)
    first = lax.axis_index("dp") % 2 == 0
    sides = jnp.where(first, grads, turned_lanes).astype(BF16)
    lane = lax.broadcasted_iota(jnp.int32, (8, LANES), 1)
    member = lax.broadcasted_iota(jnp.int32, (8, LANES), 0)
    held = jnp.zeros((8, LANES), F32)
    for query in range(queries):
        precond = jnp.concatenate([own_ref[query], swapped_ref[query]], axis=0)
        turned = jnp.dot(sides, precond, preferred_element_type=F32)
        acc = jnp.zeros((rows, LANES), F32)
        for block in range(blocks):
            at = block * LANES
            acc += turned[:, at : at + LANES] * total[:, at : at + LANES]
        acc *= weight_ref[...]
        both = acc[:8]
        for at in range(8, rows, 8):
            both += acc[at : at + 8]
        value = jnp.sum(both + pltpu.roll(both, 4, 0), axis=1, keepdims=True)
        held = jnp.where(lane == member * queries + query, value, held)
    held = jnp.where(member < 4, held, 0.0)
    line = jnp.broadcast_to(jnp.sum(held, axis=0, keepdims=True), held.shape)
    for at in range(0, out_ref.shape[0], 8):
        out_ref[at : at + 8] = line


def table_kernel(per_section, queries, got_ref, rows_ref, prior_ref, out_ref):
    sender = lax.broadcasted_iota(jnp.int32, got_ref.shape, 0) // per_section
    counted = sender <= lax.axis_index("section")
    depth = jnp.sum(jnp.where(counted, got_ref[...], 0.0), axis=0, keepdims=True)
    shape = prior_ref.shape
    own = lax.axis_index("dp") * shape[0] + lax.broadcasted_iota(jnp.int32, shape, 0)
    table = prior_ref[...]
    for member in range(rows_ref.shape[1]):
        first = member * queries
        scores = jnp.broadcast_to(depth[:, first : first + queries], shape)
        table += jnp.where(rows_ref[:, member : member + 1] == own, scores, 0.0)
    out_ref[0] = table


def packed_path(
    activations,
    out_grads,
    basis_in,
    basis_out,
    eigen_values,
    query_proj,
    lengths,
    seq_rows,
    prior_table,
):
    n, sections = lax.axis_size("dp"), lax.axis_size("section")
    micro, own_slots, hidden = activations.shape[1:]
    features = out_grads.shape[3]
    own_rows = micro * own_slots
    half = n * own_rows // 2
    rank = basis_in.shape[2]
    width = (hidden + features) // n
    lengths, seq_rows = lengths[None], seq_rows[None]
    hbm = pl.BlockSpec(memory_space=pltpu.HBM)
    params = pltpu.CompilerParams(vmem_limit_bytes=16 << 20)

    def in_hbm(*arrays):
        return [pltpu.with_memory_space_constraint(array, pltpu.HBM) for array in arrays]

    def swap(value, bit):
        return lax.ppermute(value, "dp", [(i, i ^ bit) for i in range(n)])

    pieces, basis_out = pl.pallas_call(
        pack_kernel,
        out_shape=[
            jax.ShapeDtypeStruct((n, own_rows, width), BF16),
            jax.ShapeDtypeStruct(basis_out.shape[1:], BF16),
        ],
        in_specs=[hbm] * 3,
        out_specs=[VMEM] * 2,
        scratch_shapes=[
            pltpu.VMEM((own_rows, hidden), BF16),
            pltpu.VMEM((own_rows, features), BF16),
            pltpu.SemaphoreType.DMA((3,)),
        ],
        compiler_params=params,
    )(
        *in_hbm(
            activations[0].reshape(own_rows, hidden),
            out_grads[0].reshape(own_rows, features),
            basis_out[0],
        )
    )
    got = exchange(pieces, "dp").reshape(2 * half, width)
    share = hidden // n
    mine, other = call(
        split_kernel,
        [jax.ShapeDtypeStruct((half, 2 * rank), kind) for kind in (F32, BF16)],
        jnp.dot(got[:, :share], basis_in[0], preferred_element_type=F32),
        jnp.dot(got[:, share:], basis_out, preferred_element_type=F32),
    )
    keep, gots = mine, [swap(other, 1)]
    prepared = None
    for bits in [(2, 4)] + [(1 << place,) for place in range(3, n.bit_length() - 1)]:
        ways = 1 << len(bits)
        width = rank + (keep.shape[1] - rank) // ways
        keep, *sends = call(
            functools.partial(fold_kernel, bits, 1 + len(gots)),
            [jax.ShapeDtypeStruct((half, width), kind) for kind in [F32] + [BF16] * (ways - 1)],
            keep,
            *gots,
        )
        if prepared is None:
            prepared = keep
        gots = []
        for offset, send in enumerate(sends, 1):
            gots.append(swap(send, offset * bits[0]))
    (got,) = gots
    prepare = pl.pallas_call(
        prep_kernel,
        out_shape=[
            jax.ShapeDtypeStruct(query_proj.shape[1:], BF16),
            jax.ShapeDtypeStruct((half, LANES), F32),
        ],
        in_specs=[VMEM, hbm, hbm, VMEM],
        out_specs=[VMEM] * 2,
        scratch_shapes=[
            pltpu.VMEM(query_proj.shape[1:], BF16),
            pltpu.VMEM(eigen_values.shape[1:], F32),
            pltpu.SemaphoreType.DMA((2,)),
        ],
        compiler_params=params,
    )
    precond, weight = prepare(lengths, *in_hbm(eigen_values[0], query_proj[0]), prepared)
    swapped = swap(precond, 1)
    total = n * sections
    spread = call(
        score_kernel,
        jax.ShapeDtypeStruct((total, LANES), F32),
        keep,
        got,
        precond,
        swapped,
        weight,
        seq_rows,
        prior_table,
    )
    scores = exchange(spread.reshape(total, 1, LANES), ("section", "dp")).reshape(total, LANES)
    return call(
        functools.partial(table_kernel, n, query_proj.shape[1]),
        jax.ShapeDtypeStruct((1,) + prior_table.shape, F32),
        scores,
        seq_rows,
        prior_table,
    )


def general_path(
    activations,
    out_grads,
    basis_in,
    basis_out,
    eigen_values,
    query_proj,
    lengths,
    seq_rows,
    prior_table,
):
    n = lax.axis_size("dp")
    sections = lax.axis_size("section")
    micro, own_slots, hidden = activations.shape[1:]
    features = out_grads.shape[3]
    hidden_share, feature_share = hidden // n, features // n
    own_rows = micro * own_slots
    rows = n * own_rows
    rank = basis_in.shape[2]
    share = rank // n
    queries = query_proj.shape[1]

    pieces = jnp.concatenate(
        [
            activations[0].reshape(own_rows, n, hidden_share),
            out_grads[0].reshape(own_rows, n, feature_share),
        ],
        axis=2,
    ).transpose(1, 0, 2)
    got = exchange(pieces, "dp").reshape(rows, hidden_share + feature_share)

    act_part = jnp.dot(got[:, :hidden_share], basis_in[0], preferred_element_type=F32)
    grad_part = jnp.dot(got[:, hidden_share:], basis_out[0], preferred_element_type=F32)
    parts = jnp.concatenate(
        [
            act_part.astype(BF16).reshape(rows, n, share),
            grad_part.astype(BF16).reshape(rows, n, share),
        ],
        axis=2,
    ).transpose(1, 0, 2)
    sums = jnp.sum(exchange(parts, "dp").astype(F32), axis=0)
    act_own = sums[:, :share].astype(BF16)

    row = jnp.arange(rows, dtype=jnp.int32)
    row_micro = (row // own_slots) % micro
    row_slot = (row // own_rows) * own_slots + row % own_slots
    micro_mask = row_micro[None, :] == jnp.arange(micro, dtype=jnp.int32)[:, None]
    live = jnp.any(micro_mask & (row_slot[None, :] < lengths[:, None]), axis=0)
    grad_own = jnp.where(live[:, None], sums[:, share:], 0.0).astype(BF16)

    act_all = exchange(jnp.broadcast_to(act_own[None], (n, rows, share)), "dp")
    act_proj = act_all.transpose(1, 0, 2).reshape(rows, rank)

    precond = (query_proj[0].astype(F32) / (eigen_values[0][None] + DAMPING)).astype(BF16)
    turned = jnp.einsum("ri,qij->qrj", grad_own, precond, preferred_element_type=F32)
    per_row = jnp.sum(turned * act_proj.astype(F32)[None], axis=2)
    weight = micro_mask.astype(F32) / lengths.astype(F32)[:, None]
    partial = jnp.sum(per_row[None] * weight[:, None, :], axis=2)

    total = n * sections
    spread = jnp.broadcast_to(partial.reshape(1, 1, micro * queries), (total, 1, micro * queries))
    scores = exchange(spread, ("section", "dp"))
    sender_section = jnp.arange(total, dtype=jnp.int32) // n
    counted = sender_section <= lax.axis_index("section")
    depth = jnp.sum(jnp.where(counted[:, None, None], scores, 0.0), axis=(0, 1))
    depth = depth.reshape(micro, queries)

    table_rows = prior_table.shape[0]
    first_row = lax.axis_index("dp") * table_rows
    own = first_row + jnp.arange(table_rows, dtype=jnp.int32)
    owner_mask = (seq_rows[None, :] == own[:, None]).astype(F32)
    result = prior_table + jnp.sum(owner_mask[:, :, None] * depth[None], axis=1)
    return result[None]


def per_device(*arrays):
    activations, out_grads, basis_in, _, _, query_proj, _, _, prior_table = arrays
    n = lax.axis_size("dp")
    micro, own_slots, hidden = activations.shape[1:]
    features = out_grads.shape[3]
    rank = basis_in.shape[2]
    queries = query_proj.shape[1]
    packs = (
        micro == 4
        and own_slots == 1
        and n & (n - 1) == 0
        and n >= 16
        and hidden % (n * LANES) == 0
        and features % (n * LANES) == 0
        and 2 * rank == n * LANES
        and micro * queries <= LANES
        and prior_table.shape[0] % 8 == 0
    )
    return (packed_path if packs else general_path)(*arrays)


def solution(mesh):
    return jax.shard_map(
        per_device,
        mesh=mesh,
        in_specs=(
            P("section", None, "dp", None),
            P("section", None, "dp", None),
            P("section", "dp", None),
            P("section", "dp", None),
            P("section", "dp", None),
            P("section", None, "dp", None),
            P(),
            P(),
            P("dp", None),
        ),
        out_specs=P("section", "dp", None),
        check_vma=False,
    )
```

```python
import functools

import jax
import jax.numpy as jnp
from jax import lax
from jax.experimental import pallas as pl
from jax.experimental.pallas import tpu as pltpu
from jax.sharding import PartitionSpec as P


DAMPING = 0.01
F32 = jnp.float32
BF16 = jnp.bfloat16
LANES = 128
VMEM = pl.BlockSpec(memory_space=pltpu.VMEM)


def exchange(pieces, axes):
    return lax.all_to_all(pieces, axes, split_axis=0, concat_axis=0, tiled=True)


def call(body, out_shapes, *operands):
    many = isinstance(out_shapes, (list, tuple))
    return pl.pallas_call(
        body,
        out_shape=out_shapes,
        in_specs=[VMEM] * len(operands),
        out_specs=[VMEM] * len(out_shapes) if many else VMEM,
        compiler_params=pltpu.CompilerParams(vmem_limit_bytes=16 << 20),
    )(*operands)


def pack_kernel(acts_hbm, grads_hbm, out_ref, acts_ref, grads_ref, sems):
    copies = [
        pltpu.make_async_copy(acts_hbm, acts_ref, sems.at[0]),
        pltpu.make_async_copy(grads_hbm, grads_ref, sems.at[1]),
    ]
    for copy in copies:
        copy.start(priority=1)
    peers = out_ref.shape[0]
    hidden, features = acts_ref.shape[1] // peers, grads_ref.shape[1] // peers
    copies[0].wait()
    for peer in range(peers):
        out_ref[peer, :, :hidden] = acts_ref[:, peer * hidden : (peer + 1) * hidden]
    copies[1].wait()
    for peer in range(peers):
        out_ref[peer, :, hidden:] = grads_ref[:, peer * features : (peer + 1) * features]


def prep_kernel(lengths_ref, eigen_hbm, query_hbm, after_ref, *refs):
    del after_ref
    precond_ref, weight_ref, query_ref, eigen_ref, sems = refs
    copies = [
        pltpu.make_async_copy(eigen_hbm, eigen_ref, sems.at[0]),
        pltpu.make_async_copy(query_hbm, query_ref, sems.at[1]),
    ]
    for copy in copies:
        copy.start()
    shape = weight_ref.shape
    micro = lengths_ref.shape[1]
    row = lax.axis_index("dp") % 2 * shape[0] + lax.broadcasted_iota(jnp.int32, shape, 0)
    slot, member = row // micro, row % micro
    length = jnp.zeros(shape, jnp.int32)
    for index in range(micro):
        length = jnp.where(member == index, lengths_ref[:, index : index + 1], length)
    weight_ref[...] = jnp.where(slot < length, 1.0 / length.astype(F32), 0.0)
    for copy in copies:
        copy.wait()
    damped = eigen_ref[...] + DAMPING
    for query in range(query_ref.shape[0]):
        precond_ref[query] = (query_ref[query].astype(F32) / damped).astype(BF16)


def split_kernel(acts_ref, rows_ref, basis_ref, mine_ref, other_ref):
    half, rank = mine_ref.shape[0], acts_ref.shape[1]
    first = lax.axis_index("dp") % 2 == 0
    rows = rows_ref[:, rows_ref.shape[1] - basis_ref.shape[0] :]
    grads = jnp.dot(rows, basis_ref[...], preferred_element_type=F32)
    for at, part in ((0, acts_ref[...]), (rank, grads)):
        top, bottom = part[:half], part[half:]
        mine_ref[:, at : at + rank] = jnp.where(first, top, bottom)
        other_ref[:, at : at + rank] = jnp.where(first, bottom, top).astype(BF16)


def fold_kernel(bits, count, *refs):
    total = refs[0][...]
    for got_ref in refs[1:count]:
        total += got_ref[...].astype(F32)
    outs = refs[count:]
    ways = len(outs)
    width = outs[0].shape[1]
    blocks = (total.shape[1] - width) // LANES // (ways - 1)
    rank = width - blocks * LANES
    low = [lax.axis_index("dp") // bit % 2 == 0 for bit in bits]
    for offset, out_ref in enumerate(outs):
        out_ref[:, :rank] = total[:, :rank].astype(out_ref.dtype)
        for block in range(blocks):
            at = rank + block * ways * LANES
            left = [total[:, at + way * LANES : at + (way + 1) * LANES] for way in range(ways)]
            for place, mine in enumerate(low):
                flip = offset >> place & 1
                left = [
                    jnp.where(mine, left[pair + flip], left[pair + 1 - flip])
                    for pair in range(0, len(left), 2)
                ]
            to = rank + block * LANES
            out_ref[:, to : to + LANES] = left[0].astype(out_ref.dtype)


def score_kernel(mine_ref, got_ref, own_ref, swapped_ref, weight_ref, *refs):
    out_ref = refs[-1]
    queries, share, rank = own_ref.shape
    rows = weight_ref.shape[0]
    blocks = rank // LANES
    total = mine_ref[...] + got_ref[...].astype(F32)
    grads = total[:, rank:]
    turned_lanes = pltpu.roll(grads, share, 1)
    first = lax.axis_index("dp") % 2 == 0
    sides = jnp.where(first, grads, turned_lanes).astype(BF16)
    lane = lax.broadcasted_iota(jnp.int32, (8, LANES), 1)
    member = lax.broadcasted_iota(jnp.int32, (8, LANES), 0)
    held = jnp.zeros((8, LANES), F32)
    for query in range(queries):
        precond = jnp.concatenate([own_ref[query], swapped_ref[query]], axis=0)
        turned = jnp.dot(sides, precond, preferred_element_type=F32)
        acc = jnp.zeros((rows, LANES), F32)
        for block in range(blocks):
            at = block * LANES
            acc += turned[:, at : at + LANES] * total[:, at : at + LANES]
        acc *= weight_ref[...]
        both = acc[:8]
        for at in range(8, rows, 8):
            both += acc[at : at + 8]
        value = jnp.sum(both + pltpu.roll(both, 4, 0), axis=1, keepdims=True)
        held = jnp.where(lane == member * queries + query, value, held)
    held = jnp.where(member < 4, held, 0.0)
    line = jnp.broadcast_to(jnp.sum(held, axis=0, keepdims=True), held.shape)
    for at in range(0, out_ref.shape[0], 8):
        out_ref[at : at + 8] = line


def table_kernel(per_section, queries, got_ref, rows_ref, prior_ref, out_ref):
    sender = lax.broadcasted_iota(jnp.int32, got_ref.shape, 0) // per_section
    counted = sender <= lax.axis_index("section")
    depth = jnp.sum(jnp.where(counted, got_ref[...], 0.0), axis=0, keepdims=True)
    shape = prior_ref.shape
    own = lax.axis_index("dp") * shape[0] + lax.broadcasted_iota(jnp.int32, shape, 0)
    table = prior_ref[...]
    for member in range(rows_ref.shape[1]):
        first = member * queries
        scores = jnp.broadcast_to(depth[:, first : first + queries], shape)
        table += jnp.where(rows_ref[:, member : member + 1] == own, scores, 0.0)
    out_ref[0] = table


def packed_path(
    activations,
    out_grads,
    basis_in,
    basis_out,
    eigen_values,
    query_proj,
    lengths,
    seq_rows,
    prior_table,
):
    n, sections = lax.axis_size("dp"), lax.axis_size("section")
    micro, own_slots, hidden = activations.shape[1:]
    features = out_grads.shape[3]
    own_rows = micro * own_slots
    half = n * own_rows // 2
    rank = basis_in.shape[2]
    width = (hidden + features) // n
    lengths, seq_rows = lengths[None], seq_rows[None]
    hbm = pl.BlockSpec(memory_space=pltpu.HBM)
    params = pltpu.CompilerParams(vmem_limit_bytes=16 << 20)

    def in_hbm(*arrays):
        return [pltpu.with_memory_space_constraint(array, pltpu.HBM) for array in arrays]

    def swap(value, bit):
        return lax.ppermute(value, "dp", [(i, i ^ bit) for i in range(n)])

    pieces = pl.pallas_call(
        pack_kernel,
        out_shape=jax.ShapeDtypeStruct((n, own_rows, width), BF16),
        in_specs=[hbm] * 2,
        out_specs=VMEM,
        scratch_shapes=[
            pltpu.VMEM((own_rows, hidden), BF16),
            pltpu.VMEM((own_rows, features), BF16),
            pltpu.SemaphoreType.DMA((2,)),
        ],
        compiler_params=params,
    )(
        *in_hbm(
            activations[0].reshape(own_rows, hidden),
            out_grads[0].reshape(own_rows, features),
        )
    )
    got = exchange(pieces, "dp").reshape(2 * half, width)
    share = hidden // n
    mine, other = call(
        split_kernel,
        [jax.ShapeDtypeStruct((half, 2 * rank), kind) for kind in (F32, BF16)],
        jnp.dot(got[:, :share], basis_in[0], preferred_element_type=F32),
        got,
        basis_out[0],
    )
    keep, gots = mine, [swap(other, 1)]
    prepared = None
    for bits in [(2, 4)] + [(1 << place,) for place in range(3, n.bit_length() - 1)]:
        ways = 1 << len(bits)
        width = rank + (keep.shape[1] - rank) // ways
        keep, *sends = call(
            functools.partial(fold_kernel, bits, 1 + len(gots)),
            [jax.ShapeDtypeStruct((half, width), kind) for kind in [F32] + [BF16] * (ways - 1)],
            keep,
            *gots,
        )
        if prepared is None:
            prepared = keep
        gots = []
        for offset, send in enumerate(sends, 1):
            gots.append(swap(send, offset * bits[0]))
    (got,) = gots
    prepare = pl.pallas_call(
        prep_kernel,
        out_shape=[
            jax.ShapeDtypeStruct(query_proj.shape[1:], BF16),
            jax.ShapeDtypeStruct((half, LANES), F32),
        ],
        in_specs=[VMEM, hbm, hbm, VMEM],
        out_specs=[VMEM] * 2,
        scratch_shapes=[
            pltpu.VMEM(query_proj.shape[1:], BF16),
            pltpu.VMEM(eigen_values.shape[1:], F32),
            pltpu.SemaphoreType.DMA((2,)),
        ],
        compiler_params=params,
    )
    precond, weight = prepare(lengths, *in_hbm(eigen_values[0], query_proj[0]), prepared)
    swapped = swap(precond, 1)
    total = n * sections
    spread = call(
        score_kernel,
        jax.ShapeDtypeStruct((total, LANES), F32),
        keep,
        got,
        precond,
        swapped,
        weight,
        seq_rows,
        prior_table,
    )
    scores = exchange(spread.reshape(total, 1, LANES), ("section", "dp")).reshape(total, LANES)
    return call(
        functools.partial(table_kernel, n, query_proj.shape[1]),
        jax.ShapeDtypeStruct((1,) + prior_table.shape, F32),
        scores,
        seq_rows,
        prior_table,
    )


def general_path(
    activations,
    out_grads,
    basis_in,
    basis_out,
    eigen_values,
    query_proj,
    lengths,
    seq_rows,
    prior_table,
):
    n = lax.axis_size("dp")
    sections = lax.axis_size("section")
    micro, own_slots, hidden = activations.shape[1:]
    features = out_grads.shape[3]
    hidden_share, feature_share = hidden // n, features // n
    own_rows = micro * own_slots
    rows = n * own_rows
    rank = basis_in.shape[2]
    share = rank // n
    queries = query_proj.shape[1]

    pieces = jnp.concatenate(
        [
            activations[0].reshape(own_rows, n, hidden_share),
            out_grads[0].reshape(own_rows, n, feature_share),
        ],
        axis=2,
    ).transpose(1, 0, 2)
    got = exchange(pieces, "dp").reshape(rows, hidden_share + feature_share)

    act_part = jnp.dot(got[:, :hidden_share], basis_in[0], preferred_element_type=F32)
    grad_part = jnp.dot(got[:, hidden_share:], basis_out[0], preferred_element_type=F32)
    parts = jnp.concatenate(
        [
            act_part.astype(BF16).reshape(rows, n, share),
            grad_part.astype(BF16).reshape(rows, n, share),
        ],
        axis=2,
    ).transpose(1, 0, 2)
    sums = jnp.sum(exchange(parts, "dp").astype(F32), axis=0)
    act_own = sums[:, :share].astype(BF16)

    row = jnp.arange(rows, dtype=jnp.int32)
    row_micro = (row // own_slots) % micro
    row_slot = (row // own_rows) * own_slots + row % own_slots
    micro_mask = row_micro[None, :] == jnp.arange(micro, dtype=jnp.int32)[:, None]
    live = jnp.any(micro_mask & (row_slot[None, :] < lengths[:, None]), axis=0)
    grad_own = jnp.where(live[:, None], sums[:, share:], 0.0).astype(BF16)

    act_all = exchange(jnp.broadcast_to(act_own[None], (n, rows, share)), "dp")
    act_proj = act_all.transpose(1, 0, 2).reshape(rows, rank)

    precond = (query_proj[0].astype(F32) / (eigen_values[0][None] + DAMPING)).astype(BF16)
    turned = jnp.einsum("ri,qij->qrj", grad_own, precond, preferred_element_type=F32)
    per_row = jnp.sum(turned * act_proj.astype(F32)[None], axis=2)
    weight = micro_mask.astype(F32) / lengths.astype(F32)[:, None]
    partial = jnp.sum(per_row[None] * weight[:, None, :], axis=2)

    total = n * sections
    spread = jnp.broadcast_to(partial.reshape(1, 1, micro * queries), (total, 1, micro * queries))
    scores = exchange(spread, ("section", "dp"))
    sender_section = jnp.arange(total, dtype=jnp.int32) // n
    counted = sender_section <= lax.axis_index("section")
    depth = jnp.sum(jnp.where(counted[:, None, None], scores, 0.0), axis=(0, 1))
    depth = depth.reshape(micro, queries)

    table_rows = prior_table.shape[0]
    first_row = lax.axis_index("dp") * table_rows
    own = first_row + jnp.arange(table_rows, dtype=jnp.int32)
    owner_mask = (seq_rows[None, :] == own[:, None]).astype(F32)
    result = prior_table + jnp.sum(owner_mask[:, :, None] * depth[None], axis=1)
    return result[None]


def per_device(*arrays):
    activations, out_grads, basis_in, _, _, query_proj, _, _, prior_table = arrays
    n = lax.axis_size("dp")
    micro, own_slots, hidden = activations.shape[1:]
    features = out_grads.shape[3]
    rank = basis_in.shape[2]
    queries = query_proj.shape[1]
    packs = (
        micro == 4
        and own_slots == 1
        and n & (n - 1) == 0
        and n >= 16
        and hidden % (n * LANES) == 0
        and features % (n * LANES) == 0
        and 2 * rank == n * LANES
        and micro * queries <= LANES
        and prior_table.shape[0] % 8 == 0
    )
    return (packed_path if packs else general_path)(*arrays)


def solution(mesh):
    return jax.shard_map(
        per_device,
        mesh=mesh,
        in_specs=(
            P("section", None, "dp", None),
            P("section", None, "dp", None),
            P("section", "dp", None),
            P("section", "dp", None),
            P("section", "dp", None),
            P("section", None, "dp", None),
            P(),
            P(),
            P("dp", None),
        ),
        out_specs=P("section", "dp", None),
        check_vma=False,
    )
```

```python
import functools

import jax
import jax.numpy as jnp
from jax import lax
from jax.experimental import pallas as pl
from jax.experimental.pallas import tpu as pltpu
from jax.sharding import PartitionSpec as P


DAMPING = 0.01
F32 = jnp.float32
BF16 = jnp.bfloat16
LANES = 128
VMEM = pl.BlockSpec(memory_space=pltpu.VMEM)


def exchange(pieces, axes):
    return lax.all_to_all(pieces, axes, split_axis=0, concat_axis=0, tiled=True)


def call(body, out_shapes, *operands):
    many = isinstance(out_shapes, (list, tuple))
    return pl.pallas_call(
        body,
        out_shape=out_shapes,
        in_specs=[VMEM] * len(operands),
        out_specs=[VMEM] * len(out_shapes) if many else VMEM,
        compiler_params=pltpu.CompilerParams(vmem_limit_bytes=16 << 20),
    )(*operands)


def pack_kernel(acts_hbm, grads_hbm, out_ref, acts_ref, grads_ref, sems):
    copies = [
        pltpu.make_async_copy(acts_hbm, acts_ref, sems.at[0]),
        pltpu.make_async_copy(grads_hbm, grads_ref, sems.at[1]),
    ]
    for copy in copies:
        copy.start(priority=1)
    peers = out_ref.shape[0]
    hidden, features = acts_ref.shape[1] // peers, grads_ref.shape[1] // peers
    copies[0].wait()
    for peer in range(peers):
        out_ref[peer, :, :hidden] = acts_ref[:, peer * hidden : (peer + 1) * hidden]
    copies[1].wait()
    for peer in range(peers):
        out_ref[peer, :, hidden:] = grads_ref[:, peer * features : (peer + 1) * features]


def prep_kernel(lengths_ref, eigen_hbm, query_hbm, after_ref, *refs):
    del after_ref
    precond_ref, weight_ref, query_ref, eigen_ref, sems = refs
    copies = [
        pltpu.make_async_copy(eigen_hbm, eigen_ref, sems.at[0]),
        pltpu.make_async_copy(query_hbm, query_ref, sems.at[1]),
    ]
    for copy in copies:
        copy.start()
    shape = weight_ref.shape
    micro = lengths_ref.shape[1]
    row = lax.axis_index("dp") % 2 * shape[0] + lax.broadcasted_iota(jnp.int32, shape, 0)
    slot, member = row // micro, row % micro
    length = jnp.zeros(shape, jnp.int32)
    for index in range(micro):
        length = jnp.where(member == index, lengths_ref[:, index : index + 1], length)
    weight_ref[...] = jnp.where(slot < length, 1.0 / length.astype(F32), 0.0)
    for copy in copies:
        copy.wait()
    damped = eigen_ref[...] + DAMPING
    for query in range(query_ref.shape[0]):
        precond_ref[query] = (query_ref[query].astype(F32) / damped).astype(BF16)


def split_kernel(acts_ref, rows_ref, basis_ref, mine_ref, other_ref):
    half, rank = mine_ref.shape[0], acts_ref.shape[1]
    first = lax.axis_index("dp") % 2 == 0
    rows = rows_ref[:, rows_ref.shape[1] - basis_ref.shape[0] :]
    grads = jnp.dot(rows, basis_ref[...], preferred_element_type=F32)
    for at, part in ((0, acts_ref[...]), (rank, grads)):
        top, bottom = part[:half], part[half:]
        mine_ref[:, at : at + rank] = jnp.where(first, top, bottom)
        other_ref[:, at : at + rank] = jnp.where(first, bottom, top).astype(BF16)


def fold_kernel(bits, count, *refs):
    total = refs[0][...]
    for got_ref in refs[1:count]:
        total += got_ref[...].astype(F32)
    outs = refs[count:]
    ways = len(outs)
    width = outs[0].shape[1]
    blocks = (total.shape[1] - width) // LANES // (ways - 1)
    rank = width - blocks * LANES
    low = [lax.axis_index("dp") // bit % 2 == 0 for bit in bits]
    for offset, out_ref in enumerate(outs):
        out_ref[:, :rank] = total[:, :rank].astype(out_ref.dtype)
        for block in range(blocks):
            at = rank + block * ways * LANES
            left = [total[:, at + way * LANES : at + (way + 1) * LANES] for way in range(ways)]
            for place, mine in enumerate(low):
                flip = offset >> place & 1
                left = [
                    jnp.where(mine, left[pair + flip], left[pair + 1 - flip])
                    for pair in range(0, len(left), 2)
                ]
            to = rank + block * LANES
            out_ref[:, to : to + LANES] = left[0].astype(out_ref.dtype)


def score_kernel(mine_ref, got_ref, own_ref, swapped_ref, weight_ref, *refs):
    out_ref = refs[-1]
    queries, share, rank = own_ref.shape
    rows = weight_ref.shape[0]
    blocks = rank // LANES
    total = mine_ref[...] + got_ref[...].astype(F32)
    grads = total[:, rank:]
    turned_lanes = pltpu.roll(grads, share, 1)
    first = lax.axis_index("dp") % 2 == 0
    sides = jnp.where(first, grads, turned_lanes).astype(BF16)
    lane = lax.broadcasted_iota(jnp.int32, (8, LANES), 1)
    member = lax.broadcasted_iota(jnp.int32, (8, LANES), 0)
    held = jnp.zeros((8, LANES), F32)
    for query in range(queries):
        precond = jnp.concatenate([own_ref[query], swapped_ref[query]], axis=0)
        turned = jnp.dot(sides, precond, preferred_element_type=F32)
        acc = jnp.zeros((rows, LANES), F32)
        for block in range(blocks):
            at = block * LANES
            acc += turned[:, at : at + LANES] * total[:, at : at + LANES]
        acc *= weight_ref[...]
        both = acc[:8]
        for at in range(8, rows, 8):
            both += acc[at : at + 8]
        value = jnp.sum(both + pltpu.roll(both, 4, 0), axis=1, keepdims=True)
        held = jnp.where(lane == member * queries + query, value, held)
    held = jnp.where(member < 4, held, 0.0)
    line = jnp.broadcast_to(jnp.sum(held, axis=0, keepdims=True), held.shape)
    for at in range(0, out_ref.shape[0], 8):
        out_ref[at : at + 8] = line


def table_kernel(per_section, queries, got_ref, rows_ref, prior_ref, out_hbm, table_ref, sem):
    sender = lax.broadcasted_iota(jnp.int32, got_ref.shape, 0) // per_section
    counted = sender <= lax.axis_index("section")
    depth = jnp.sum(jnp.where(counted, got_ref[...], 0.0), axis=0, keepdims=True)
    shape = prior_ref.shape
    own = lax.axis_index("dp") * shape[0] + lax.broadcasted_iota(jnp.int32, shape, 0)
    table = prior_ref[...]
    for member in range(rows_ref.shape[1]):
        first = member * queries
        scores = jnp.broadcast_to(depth[:, first : first + queries], shape)
        table += jnp.where(rows_ref[:, member : member + 1] == own, scores, 0.0)
    table_ref[0] = table
    copy = pltpu.make_async_copy(table_ref, out_hbm, sem)
    copy.start()
    copy.wait()


def packed_path(
    activations,
    out_grads,
    basis_in,
    basis_out,
    eigen_values,
    query_proj,
    lengths,
    seq_rows,
    prior_table,
):
    n, sections = lax.axis_size("dp"), lax.axis_size("section")
    micro, own_slots, hidden = activations.shape[1:]
    features = out_grads.shape[3]
    own_rows = micro * own_slots
    half = n * own_rows // 2
    rank = basis_in.shape[2]
    width = (hidden + features) // n
    lengths, seq_rows = lengths[None], seq_rows[None]
    hbm = pl.BlockSpec(memory_space=pltpu.HBM)
    params = pltpu.CompilerParams(vmem_limit_bytes=16 << 20)

    def in_hbm(*arrays):
        return [pltpu.with_memory_space_constraint(array, pltpu.HBM) for array in arrays]

    def swap(value, bit):
        return lax.ppermute(value, "dp", [(i, i ^ bit) for i in range(n)])

    pieces = pl.pallas_call(
        pack_kernel,
        out_shape=jax.ShapeDtypeStruct((n, own_rows, width), BF16),
        in_specs=[hbm] * 2,
        out_specs=VMEM,
        scratch_shapes=[
            pltpu.VMEM((own_rows, hidden), BF16),
            pltpu.VMEM((own_rows, features), BF16),
            pltpu.SemaphoreType.DMA((2,)),
        ],
        compiler_params=params,
    )(
        *in_hbm(
            activations[0].reshape(own_rows, hidden),
            out_grads[0].reshape(own_rows, features),
        )
    )
    got = exchange(pieces, "dp").reshape(2 * half, width)
    share = hidden // n
    mine, other = call(
        split_kernel,
        [jax.ShapeDtypeStruct((half, 2 * rank), kind) for kind in (F32, BF16)],
        jnp.dot(got[:, :share], basis_in[0], preferred_element_type=F32),
        got,
        basis_out[0],
    )
    keep, gots = mine, [swap(other, 1)]
    prepared = None
    for bits in [(2, 4)] + [(1 << place,) for place in range(3, n.bit_length() - 1)]:
        ways = 1 << len(bits)
        width = rank + (keep.shape[1] - rank) // ways
        keep, *sends = call(
            functools.partial(fold_kernel, bits, 1 + len(gots)),
            [jax.ShapeDtypeStruct((half, width), kind) for kind in [F32] + [BF16] * (ways - 1)],
            keep,
            *gots,
        )
        if prepared is None:
            prepared = keep
        gots = []
        for offset, send in enumerate(sends, 1):
            gots.append(swap(send, offset * bits[0]))
    (got,) = gots
    prepare = pl.pallas_call(
        prep_kernel,
        out_shape=[
            jax.ShapeDtypeStruct(query_proj.shape[1:], BF16),
            jax.ShapeDtypeStruct((half, LANES), F32),
        ],
        in_specs=[VMEM, hbm, hbm, VMEM],
        out_specs=[VMEM] * 2,
        scratch_shapes=[
            pltpu.VMEM(query_proj.shape[1:], BF16),
            pltpu.VMEM(eigen_values.shape[1:], F32),
            pltpu.SemaphoreType.DMA((2,)),
        ],
        compiler_params=params,
    )
    precond, weight = prepare(lengths, *in_hbm(eigen_values[0], query_proj[0]), prepared)
    swapped = swap(precond, 1)
    total = n * sections
    spread = call(
        score_kernel,
        jax.ShapeDtypeStruct((total, LANES), F32),
        keep,
        got,
        precond,
        swapped,
        weight,
        seq_rows,
        prior_table,
    )
    scores = exchange(spread.reshape(total, 1, LANES), ("section", "dp")).reshape(total, LANES)
    return pl.pallas_call(
        functools.partial(table_kernel, n, query_proj.shape[1]),
        out_shape=jax.ShapeDtypeStruct((1,) + prior_table.shape, F32),
        in_specs=[VMEM] * 3,
        out_specs=hbm,
        scratch_shapes=[
            pltpu.VMEM((1,) + prior_table.shape, F32),
            pltpu.SemaphoreType.DMA,
        ],
        compiler_params=params,
    )(scores, seq_rows, prior_table)


def general_path(
    activations,
    out_grads,
    basis_in,
    basis_out,
    eigen_values,
    query_proj,
    lengths,
    seq_rows,
    prior_table,
):
    n = lax.axis_size("dp")
    sections = lax.axis_size("section")
    micro, own_slots, hidden = activations.shape[1:]
    features = out_grads.shape[3]
    hidden_share, feature_share = hidden // n, features // n
    own_rows = micro * own_slots
    rows = n * own_rows
    rank = basis_in.shape[2]
    share = rank // n
    queries = query_proj.shape[1]

    pieces = jnp.concatenate(
        [
            activations[0].reshape(own_rows, n, hidden_share),
            out_grads[0].reshape(own_rows, n, feature_share),
        ],
        axis=2,
    ).transpose(1, 0, 2)
    got = exchange(pieces, "dp").reshape(rows, hidden_share + feature_share)

    act_part = jnp.dot(got[:, :hidden_share], basis_in[0], preferred_element_type=F32)
    grad_part = jnp.dot(got[:, hidden_share:], basis_out[0], preferred_element_type=F32)
    parts = jnp.concatenate(
        [
            act_part.astype(BF16).reshape(rows, n, share),
            grad_part.astype(BF16).reshape(rows, n, share),
        ],
        axis=2,
    ).transpose(1, 0, 2)
    sums = jnp.sum(exchange(parts, "dp").astype(F32), axis=0)
    act_own = sums[:, :share].astype(BF16)

    row = jnp.arange(rows, dtype=jnp.int32)
    row_micro = (row // own_slots) % micro
    row_slot = (row // own_rows) * own_slots + row % own_slots
    micro_mask = row_micro[None, :] == jnp.arange(micro, dtype=jnp.int32)[:, None]
    live = jnp.any(micro_mask & (row_slot[None, :] < lengths[:, None]), axis=0)
    grad_own = jnp.where(live[:, None], sums[:, share:], 0.0).astype(BF16)

    act_all = exchange(jnp.broadcast_to(act_own[None], (n, rows, share)), "dp")
    act_proj = act_all.transpose(1, 0, 2).reshape(rows, rank)

    precond = (query_proj[0].astype(F32) / (eigen_values[0][None] + DAMPING)).astype(BF16)
    turned = jnp.einsum("ri,qij->qrj", grad_own, precond, preferred_element_type=F32)
    per_row = jnp.sum(turned * act_proj.astype(F32)[None], axis=2)
    weight = micro_mask.astype(F32) / lengths.astype(F32)[:, None]
    partial = jnp.sum(per_row[None] * weight[:, None, :], axis=2)

    total = n * sections
    spread = jnp.broadcast_to(partial.reshape(1, 1, micro * queries), (total, 1, micro * queries))
    scores = exchange(spread, ("section", "dp"))
    sender_section = jnp.arange(total, dtype=jnp.int32) // n
    counted = sender_section <= lax.axis_index("section")
    depth = jnp.sum(jnp.where(counted[:, None, None], scores, 0.0), axis=(0, 1))
    depth = depth.reshape(micro, queries)

    table_rows = prior_table.shape[0]
    first_row = lax.axis_index("dp") * table_rows
    own = first_row + jnp.arange(table_rows, dtype=jnp.int32)
    owner_mask = (seq_rows[None, :] == own[:, None]).astype(F32)
    result = prior_table + jnp.sum(owner_mask[:, :, None] * depth[None], axis=1)
    return result[None]


def per_device(*arrays):
    activations, out_grads, basis_in, _, _, query_proj, _, _, prior_table = arrays
    n = lax.axis_size("dp")
    micro, own_slots, hidden = activations.shape[1:]
    features = out_grads.shape[3]
    rank = basis_in.shape[2]
    queries = query_proj.shape[1]
    packs = (
        micro == 4
        and own_slots == 1
        and n & (n - 1) == 0
        and n >= 16
        and hidden % (n * LANES) == 0
        and features % (n * LANES) == 0
        and 2 * rank == n * LANES
        and micro * queries <= LANES
        and prior_table.shape[0] % 8 == 0
    )
    return (packed_path if packs else general_path)(*arrays)


def solution(mesh):
    return jax.shard_map(
        per_device,
        mesh=mesh,
        in_specs=(
            P("section", None, "dp", None),
            P("section", None, "dp", None),
            P("section", "dp", None),
            P("section", "dp", None),
            P("section", "dp", None),
            P("section", None, "dp", None),
            P(),
            P(),
            P("dp", None),
        ),
        out_specs=P("section", "dp", None),
        check_vma=False,
    )
```
